32 devices in a mesh: section: 4 (over z), dp: 2 (over x), space: 4 (over y, core).
Axes of the slice: x: 2, y: 2, z: 4, core: 2. Of those that a mesh axis runs over, the one named last changes fastest.
Arguments:
- enc_input: bfloat16 [4, 2, 32, 8, 8, 128], P('section', 'dp', None, 'space'), may hold values from -6 to 6
- dec_input: bfloat16 [4, 2, 32, 8, 8, 128], P('section', 'dp', None, None, 'space'), may hold values from -6 to 6
- dec_cotangent: bfloat16 [4, 2, 32, 8, 8, 128], P('section', 'dp', None, None, 'space'), may hold values from -6 to 6
- deep_cotangent: bfloat16 [4, 2, 32, 8, 8, 128], P('section', 'dp', None, 'space'), may hold values from -6 to 6
- enc_weight: bfloat16 [4, 27, 32, 32], P('section'), may hold values from -0.21875 to 0.21875
- dec_weight: bfloat16 [4, 27, 32, 64], P('section'), may hold values from -0.15625 to 0.15625
- enc_gain: float32 [4, 32], P('section'), may hold values from 0.25 to 1.75
- enc_bias: float32 [4, 32], P('section'), may hold values from -2 to 2
- dec_gain: float32 [4, 32], P('section'), may hold values from 0.25 to 1.75
- dec_bias: float32 [4, 32], P('section'), may hold values from -2 to 2
Outputs:
- enc_handoff: bfloat16 [4, 2, 32, 8, 8, 128], P('section', 'dp', None, 'space')
- dec_handoff: bfloat16 [4, 2, 32, 8, 8, 128], P('section', 'dp', None, None, 'space')
- enc_weight_grad: float32 [4, 27648], P('section', ('dp', 'space'))
- dec_weight_grad: float32 [4, 55296], P('section', ('dp', 'space'))
The draws below stay inside these ranges and needn't reach their ends.
All inputs are finite; a program needn't handle non-finite values.
Results may differ from the reference program's by a relative error of at most 0.0075.
Values may be sent and summed in bfloat16 or wider, within the bound.
No kernel may reach another device: no remote copies, remote signals or barrier semaphores. Data moves between devices by JAX's collectives and lax.ppermute only.
A program may use at most 64 MiB of HBM per device.

```python
import math
import jax
import jax.numpy as jnp
from jax import lax

C = 32
W = 128
SECTIONS = 4
BATCH = 2
D = 8
H = 8
N_DP = 2


def levels(key, shape, cuts, least, top_value):
    loudness, own = 1.0, jax.random.fold_in(key, 6)
    for axis_at, shards_of in cuts:
        draws = jnp.exp(jax.random.uniform(jax.random.fold_in(own, axis_at), (shards_of,), jnp.float32, least / len(cuts), top_value / len(cuts)))
        loudness = loudness * jnp.repeat(draws, shape[axis_at] // shards_of).reshape([-1 if axis == axis_at else 1 for axis in range(len(shape))])
    return loudness


def centred(rng, dims, scale, limit, cuts=(), held_as=jnp.bfloat16):
    values = scale * jax.random.normal(rng, dims, jnp.float32)
    if cuts:
        values = values * levels(rng, dims, cuts, -0.22, 0.18)
    return jnp.clip(values, -limit, limit).astype(held_as)


def setup_inputs(seed: int = 0) -> dict:
    streams_of = jax.random.split(jax.random.key(seed), 11)
    enc_input = centred(streams_of[0], (SECTIONS, BATCH, C, D, H, W), 1.0, 6.0, ((0, 4), (1, 2), (3, 4)))
    dec_input = centred(streams_of[1], (SECTIONS, BATCH, C, D, H, W), 1.0, 6.0, ((0, 4), (1, 2), (4, 4)))
    dec_cotangent = centred(streams_of[2], (SECTIONS, BATCH, C, D, H, W), 1.0, 6.0, ((0, 4), (1, 2), (4, 4)))
    deep_cotangent = centred(streams_of[3], (SECTIONS, BATCH, C, D, H, W), 1.0, 6.0, ((0, 4), (1, 2), (3, 4)))
    enc_weight = centred(streams_of[4], (SECTIONS, 27, C, C), (27 * C) ** -0.5, 0.21875, ((0, 4),))
    dec_weight = centred(streams_of[5], (SECTIONS, 27, C, 2 * C), (54 * C) ** -0.5, 0.15625, ((0, 4),))
    enc_gain = jnp.clip(1.0 + 0.15 * jax.random.normal(streams_of[6], (SECTIONS, C), jnp.float32), 0.25, 1.75)
    enc_bias = centred(streams_of[7], (SECTIONS, C), 0.5, 2.0, ((0, 4),), jnp.float32)
    dec_gain = jnp.clip(1.0 + 0.15 * jax.random.normal(streams_of[8], (SECTIONS, C), jnp.float32), 0.25, 1.75)
    dec_bias = centred(streams_of[9], (SECTIONS, C), 0.5, 2.0, ((0, 4),), jnp.float32)
    return dict(enc_input=enc_input, dec_input=dec_input, dec_cotangent=dec_cotangent, deep_cotangent=deep_cotangent, enc_weight=enc_weight, dec_weight=dec_weight, enc_gain=enc_gain, enc_bias=enc_bias, dec_gain=dec_gain, dec_bias=dec_bias)


EPS = 1e-05

def convolve(padded, weights):
    depth_cells = padded.shape[1] - 2
    height_cells = padded.shape[2] - 2
    width_cells = padded.shape[3] - 2
    summed = jnp.zeros((weights.shape[1], depth_cells, height_cells, width_cells), jnp.float32)
    for tap_index in range(27):
        depth_tap = tap_index // 9
        height_tap = tap_index // 3 % 3
        width_tap = tap_index % 3
        window = padded[:, depth_tap:depth_tap + depth_cells, height_tap:height_tap + height_cells, width_tap:width_tap + width_cells]
        summed = summed + jnp.einsum('oi,idhw->odhw', weights[tap_index].astype(jnp.float32), window.astype(jnp.float32))
    return summed

def weight_terms(padded, cotangent):
    depth_cells = cotangent.shape[1]
    height_cells = cotangent.shape[2]
    width_cells = cotangent.shape[3]
    pieces = []
    for tap_index in range(27):
        depth_tap = tap_index // 9
        height_tap = tap_index // 3 % 3
        width_tap = tap_index % 3
        window = padded[:, depth_tap:depth_tap + depth_cells, height_tap:height_tap + height_cells, width_tap:width_tap + width_cells]
        pieces.append(jnp.einsum('odhw,idhw->oi', cotangent.astype(jnp.float32), window.astype(jnp.float32)))
    return jnp.stack(pieces)

def standardize(values):
    mean_value = lax.optimization_barrier(jnp.mean(values, axis=(1, 2, 3)))
    variance = lax.optimization_barrier(jnp.mean(values * values, axis=(1, 2, 3))) - mean_value * mean_value
    scaling = lax.rsqrt(variance + EPS)
    return ((values - mean_value[:, None, None, None]) * scaling[:, None, None, None], scaling)

def pad_all(volume):
    return jnp.pad(volume, ((0, 0), (1, 1), (1, 1), (1, 1)))

def one_crop(enc_in, dec_in, cot_in, deep_in, enc_w, dec_w, enc_g, enc_b, dec_g, dec_b):
    enc_padded = pad_all(enc_in)
    enc_pre = convolve(enc_padded, enc_w)
    enc_hat, enc_scale = standardize(enc_pre)
    enc_normed = enc_g[:, None, None, None] * enc_hat + enc_b[:, None, None, None]
    skip_act = jnp.maximum(enc_normed, 0.0).astype(jnp.bfloat16)
    joined = jnp.concatenate([dec_in, skip_act], axis=0)
    dec_padded = pad_all(joined)
    dec_pre = convolve(dec_padded, dec_w)
    dec_hat, unused_scale = standardize(dec_pre)
    dec_act = jnp.maximum(dec_g[:, None, None, None] * dec_hat + dec_b[:, None, None, None], 0.0).astype(jnp.bfloat16)
    dec_grad = weight_terms(dec_padded, cot_in)
    flipped = jnp.swapaxes(dec_w[::-1, :, C:], 1, 2)
    skip_grad = convolve(pad_all(cot_in), flipped).astype(jnp.bfloat16)
    upstream = skip_grad.astype(jnp.float32) + deep_in.astype(jnp.float32)
    gated = jnp.where(enc_normed > 0, upstream, 0.0) * enc_g[:, None, None, None]
    first_mean = lax.optimization_barrier(jnp.mean(gated, axis=(1, 2, 3)))[:, None, None, None]
    second_mean = lax.optimization_barrier(jnp.mean(gated * enc_hat, axis=(1, 2, 3)))[:, None, None, None]
    enc_pre_grad = ((gated - first_mean - enc_hat * second_mean) * enc_scale[:, None, None, None]).astype(jnp.bfloat16)
    enc_grad = weight_terms(enc_padded, enc_pre_grad)
    return (skip_act, dec_act, enc_grad, dec_grad)

def reference(enc_input, dec_input, dec_cotangent, deep_cotangent, enc_weight, dec_weight, enc_gain, enc_bias, dec_gain, dec_bias):
    grad_scale = 1.0 / math.sqrt(N_DP * D * H * W)

    def one_section(section_args):
        enc_in, dec_in, cot_in, deep_in, enc_w, dec_w, enc_g, enc_b, dec_g, dec_b = section_args

        def run_crop(crop_args):
            return one_crop(crop_args[0], crop_args[1], crop_args[2], crop_args[3], enc_w, dec_w, enc_g, enc_b, dec_g, dec_b)
        skips, decoded, enc_grads, dec_grads = lax.map(run_crop, (enc_in, dec_in, cot_in, deep_in))
        enc_total = lax.optimization_barrier(jnp.sum(enc_grads, axis=0)).reshape(-1) * grad_scale
        dec_total = lax.optimization_barrier(jnp.sum(dec_grads, axis=0)).reshape(-1) * grad_scale
        return (skips, decoded, enc_total, dec_total)
    skips, decoded, enc_total, dec_total = lax.map(one_section, (enc_input, dec_input, dec_cotangent, deep_cotangent, enc_weight, dec_weight, enc_gain, enc_bias, dec_gain, dec_bias))
    enc_handoff = jnp.concatenate([jnp.zeros_like(skips[:1]), skips[:-1]], axis=0)
    dec_handoff = jnp.concatenate([decoded[1:], jnp.zeros_like(decoded[:1])], axis=0)
    return (enc_handoff, dec_handoff, enc_total, dec_total)
```

```python
import functools
import math

import jax
import jax.numpy as jnp
from jax import lax
from jax.experimental import pallas as pl
from jax.experimental.pallas import tpu as pltpu
from jax.sharding import PartitionSpec as P

EPS = 1e-05
TAPS = 3
LIMIT = 20 * 1024 * 1024
BF16 = jnp.bfloat16
F32 = jnp.float32


def vmem():
    return pl.BlockSpec(memory_space=pltpu.VMEM)


def smem():
    return pl.BlockSpec(memory_space=pltpu.SMEM)


def call(body, outs, scratch, flops, name):
    return pl.pallas_call(
        body,
        out_shape=outs,
        scratch_shapes=scratch,
        compiler_params=pltpu.CompilerParams(vmem_limit_bytes=LIMIT),
        cost_estimate=pl.CostEstimate(flops=flops, bytes_accessed=1 << 20, transcendentals=0),
        name=name,
    )


def width_shifts(rows):
    width = rows.shape[1]
    lane = lax.broadcasted_iota(jnp.int32, rows.shape, 1)
    wide = rows.astype(F32)
    left = jnp.where(lane == 0, 0.0, pltpu.roll(wide, 1, 1)).astype(BF16)
    right = jnp.where(lane == width - 1, 0.0, pltpu.roll(wide, width - 1, 1)).astype(BF16)
    return (left, rows, right)


def weights_kernel(channels, heights, strips_ref, out_ref):
    rows = channels * heights
    lanes = strips_ref.shape[-1]
    lane = lax.broadcasted_iota(jnp.int32, (channels, lanes), 1)

    @pl.loop(0, strips_ref.shape[0] * TAPS)
    def _(step):
        kind = step // TAPS
        depth_tap = step % TAPS
        for width_tap in range(TAPS):
            strip = strips_ref[kind, depth_tap, width_tap].astype(F32)
            turned = {}
            for height in range(heights):
                offset = channels * (height - 1)
                turn = offset % lanes
                if turn not in turned:
                    turned[turn] = pltpu.roll(strip, turn, 1) if turn else strip
                for tile in range(rows // lanes):
                    place = lane + (lanes * tile - offset)
                    block = jnp.where((place >= 0) & (place < TAPS * channels), turned[turn], 0.0)
                    first = pl.multiple_of(depth_tap * rows + channels * height, channels)
                    out_ref[
                        kind,
                        pl.ds(first, channels),
                        width_tap * rows + tile * lanes : width_tap * rows + (tile + 1) * lanes,
                    ] = block.astype(BF16)


def spread_depth(me, pieces, shifted_ref):
    rows = shifted_ref.shape[1] // TAPS
    depth = pieces[0].shape[0] // rows
    for distance, piece in enumerate(pieces):
        owner = me ^ distance
        for layer in range(depth):
            for tap, block in enumerate(width_shifts(piece[layer * rows : (layer + 1) * rows, :])):
                shifted_ref[owner * depth + layer, tap * rows : (tap + 1) * rows, :] = block


def spread_height(me, pieces, shifted_ref):
    depth = shifted_ref.shape[0]
    rows = shifted_ref.shape[1] // TAPS
    part = pieces[0].shape[0] // depth
    for distance, piece in enumerate(pieces):
        owner = me ^ distance

        @pl.loop(0, depth)
        def _(layer, piece=piece, owner=owner):
            cells = piece[pl.ds(pl.multiple_of(layer * part, part), part), :]
            for tap, block in enumerate(width_shifts(cells)):
                first = pl.multiple_of(tap * rows + owner * part, part)
                shifted_ref[layer, pl.ds(first, part), :] = block


def taps_product(pairs, parts_ref):
    depth = parts_ref.shape[0] - 2
    rows = parts_ref.shape[2]
    width = parts_ref.shape[3]
    for tap in range(TAPS):
        parts_ref[0, tap] = jnp.zeros((rows, width), F32)
        parts_ref[depth + 1, tap] = jnp.zeros((rows, width), F32)

    @pl.loop(0, depth // 2)
    def _(step):
        total = None
        for weights_ref, kind, shifted_ref in pairs:
            cells = jnp.concatenate([shifted_ref[2 * step], shifted_ref[2 * step + 1]], axis=1)
            product = jnp.dot(weights_ref[kind], cells, preferred_element_type=F32)
            total = product if total is None else total + product
        for tap in range(TAPS):
            block = total[tap * rows : (tap + 1) * rows]
            parts_ref[2 * step + 1, tap] = block[:, :width]
            parts_ref[2 * step + 2, tap] = block[:, width:]


def combined(parts_ref, layer):
    total = parts_ref[layer, 0]
    for tap in range(1, TAPS):
        total = total + parts_ref[layer + tap, tap]
    return total


def over_channels(sums, channels):
    total = sums[:channels]
    for first in range(channels, sums.shape[0], channels):
        total = total + sums[first : first + channels]
    return jnp.sum(total, axis=1, keepdims=True)


def tiled(values, count):
    return jnp.concatenate([values] * count, axis=0)


def normalized(parts_ref, pre_ref, sums_ref, channels):
    depth, rows, width = pre_ref.shape
    sums_ref[...] = jnp.zeros_like(sums_ref)

    @pl.loop(0, depth)
    def _(layer):
        pre = combined(parts_ref, layer)
        pre_ref[layer] = pre
        sums_ref[0] += pre
        sums_ref[1] += pre * pre

    cells = depth * (rows // channels) * width
    mean = over_channels(sums_ref[0], channels) * (1.0 / cells)
    square = over_channels(sums_ref[1], channels) * (1.0 / cells)
    return mean, lax.rsqrt(square - mean * mean + EPS)


def enc_kernel(
    channels, me_ref, p0, p1, p2, p3, weights_ref, gain_ref, bias_ref,
    shifted_ref, hat_ref, skip_ref, own_ref, scale_ref, parts_ref, pre_ref, sums_ref,
):
    me = me_ref[0]
    depth, rows, width = pre_ref.shape
    spread_depth(me, (p0, p1, p2, p3), shifted_ref)
    taps_product([(weights_ref, 0, shifted_ref)], parts_ref)
    mean, scale = normalized(parts_ref, pre_ref, sums_ref, channels)
    scale_ref[...] = jnp.broadcast_to(scale, scale_ref.shape)
    count = rows // channels
    means, scales = tiled(mean, count), tiled(scale, count)
    gains, biases = tiled(gain_ref[:, :1], count), tiled(bias_ref[:, :1], count)

    @pl.loop(0, depth)
    def _(layer):
        hat = (pre_ref[layer] - means) * scales
        hat_ref[layer] = hat
        skip_ref[layer] = jnp.maximum(gains * hat + biases, 0.0).astype(BF16)

    layers = own_ref.shape[0]
    for layer in range(layers):
        own_ref[layer] = skip_ref[me * layers + layer]


def skip_grad_kernel(me_ref, p0, p1, p2, p3, weights_ref, grad_ref, cot_ref, shifted_ref, parts_ref):
    rows = grad_ref.shape[1]
    spread_height(me_ref[0], (p0, p1, p2, p3), shifted_ref)
    taps_product([(weights_ref, 3, shifted_ref)], parts_ref)

    @pl.loop(0, grad_ref.shape[0])
    def _(layer):
        grad_ref[layer] = combined(parts_ref, layer).astype(BF16)
        cot_ref[layer] = shifted_ref[layer, rows : 2 * rows, :]


def dec_kernel(
    channels, me_ref, p0, p1, p2, p3, skip_ref, weights_ref, gain_ref, bias_ref,
    own_ref, up_ref, down_ref, parts_ref, pre_ref, sums_ref,
):
    me = me_ref[0]
    depth, rows, width = pre_ref.shape
    spread_height(me, (p0, p1, p2, p3), up_ref)

    @pl.loop(0, depth)
    def _(layer):
        for tap, block in enumerate(width_shifts(skip_ref[layer])):
            down_ref[layer, tap * rows : (tap + 1) * rows, :] = block

    taps_product([(weights_ref, 1, up_ref), (weights_ref, 2, down_ref)], parts_ref)
    mean, scale = normalized(parts_ref, pre_ref, sums_ref, channels)
    part = own_ref.shape[1]
    count = part // channels
    means, scales = tiled(mean, count), tiled(scale, count)
    gains, biases = tiled(gain_ref[:, :1], count), tiled(bias_ref[:, :1], count)

    @pl.loop(0, depth)
    def _(layer):
        pre = pre_ref[layer, pl.ds(pl.multiple_of(me * part, part), part), :]
        hat = (pre - means) * scales
        own_ref[layer] = jnp.maximum(gains * hat + biases, 0.0).astype(BF16)


def outer_sums(channels, padded_ref, shifted_refs, sums_ref):
    depth = shifted_refs[0].shape[0]
    rows = shifted_refs[0].shape[1] // TAPS
    lanes = len(shifted_refs) * TAPS * channels

    @pl.loop(0, rows // channels)
    def _(height):
        left = []
        for depth_tap in range(TAPS):
            for height_tap in range(TAPS):
                first = pl.multiple_of((height + 2 - height_tap) * channels, channels)
                left.append(
                    jnp.concatenate(
                        [
                            padded_ref[layer + 2 - depth_tap, pl.ds(first, channels), :]
                            for layer in range(depth)
                        ],
                        axis=1,
                    )
                )
        right = []
        for width_tap in range(TAPS):
            for shifted_ref in shifted_refs:
                first = pl.multiple_of(width_tap * rows + height * channels, channels)
                right.append(
                    jnp.concatenate(
                        [shifted_ref[layer, pl.ds(first, channels), :] for layer in range(depth)], axis=1
                    )
                )
        product = lax.dot_general(
            jnp.concatenate(left, axis=0),
            jnp.concatenate(right, axis=0),
            (((1,), (1,)), ((), ())),
            preferred_element_type=F32,
        )

        for tile in range(sums_ref.shape[0]):
            block = product[:, tile * 128 : min(lanes, (tile + 1) * 128)]
            old = sums_ref[tile, :, : block.shape[1]]
            sums_ref[tile, :, : block.shape[1]] = jnp.where(height == 0, 0.0, old) + block


def flattened(channels, sources, factor, sums_ref, flat_ref):
    lanes = flat_ref.shape[1]
    span = sources * channels
    merged = lanes // span
    count = channels // merged
    lane = lax.broadcasted_iota(jnp.int32, (count, lanes), 1)
    for outer in range(TAPS * TAPS):
        for width_tap in range(TAPS):
            first = width_tap * span
            tile, inner = first // lanes, first % lanes
            total = None
            for row in range(merged):
                block = sums_ref[tile, pl.ds(outer * channels + row, count, stride=merged), :]
                turn = (row * span - inner) % lanes
                block = pltpu.roll(block, turn, 1) if turn else block
                total = block if total is None else jnp.where(lane >= row * span, block, total)
            start = (outer * TAPS + width_tap) * count
            flat_ref[start : start + count, :] = total * factor


def padded_cells(channels, cells_ref, padded_ref):
    depth, rows, width = cells_ref.shape
    padded_ref[...] = jnp.zeros_like(padded_ref)

    @pl.loop(0, depth)
    def _(layer):
        padded_ref[layer + 1, channels : channels + rows, :] = cells_ref[layer]


def dec_grad_kernel(channels, factor, cot_ref, up_ref, down_ref, flat_ref, padded_ref, sums_ref):
    padded_cells(channels, cot_ref, padded_ref)
    outer_sums(channels, padded_ref, (up_ref, down_ref), sums_ref)
    flattened(channels, 2, factor, sums_ref, flat_ref)


def enc_grad_kernel(
    channels, factor, me_ref, p0, p1, p2, p3, grad_ref, hat_ref, scale_ref, gain_ref, bias_ref, shifted_ref,
    flat_ref, gated_ref, acc_ref, padded_ref, sums_ref,
):
    me = me_ref[0]
    depth, rows, width = hat_ref.shape
    count = rows // channels
    gains, biases = tiled(gain_ref[:, :1], count), tiled(bias_ref[:, :1], count)
    acc_ref[...] = jnp.zeros_like(acc_ref)
    layers = p0.shape[0] // rows
    for distance, piece in enumerate((p0, p1, p2, p3)):
        owner = me ^ distance
        for inner in range(layers):
            layer = owner * layers + inner
            hat = hat_ref[layer]
            upstream = grad_ref[layer].astype(F32) + piece[inner * rows : (inner + 1) * rows, :].astype(F32)
            gated = jnp.where(gains * hat + biases > 0, upstream, 0.0) * gains
            gated_ref[layer] = gated
            acc_ref[0] += gated
            acc_ref[1] += gated * hat
    cells = depth * count * width
    first = tiled(over_channels(acc_ref[0], channels) * (1.0 / cells), count)
    second = tiled(over_channels(acc_ref[1], channels) * (1.0 / cells), count)
    scales = tiled(scale_ref[:, :1], count)
    padded_ref[...] = jnp.zeros_like(padded_ref)

    @pl.loop(0, depth)
    def _(layer):
        grad = (gated_ref[layer] - first - hat_ref[layer] * second) * scales
        padded_ref[layer + 1, channels : channels + rows, :] = grad.astype(BF16)

    outer_sums(channels, padded_ref, (shifted_ref,), sums_ref)
    flattened(channels, 1, factor, sums_ref, flat_ref)


def gathered(piece, axis):
    count = lax.axis_size(axis)
    pieces = {0: piece}
    distance = count // 2
    while distance:
        route = [(i, i ^ distance) for i in range(count)]
        for known in list(pieces):
            pieces[known ^ distance] = lax.ppermute(pieces[known], axis, route)
        distance //= 2
    return [pieces[i] for i in range(count)]


def shifted_2(block, axis, distance):
    devices = range(lax.axis_size(axis))
    route = [(i - distance, i) for i in devices if i - distance in devices]
    return lax.ppermute(block, axis, route)


def strips(weights, channels):
    grouped = weights.reshape(TAPS, TAPS, TAPS, channels, channels).transpose(0, 2, 3, 1, 4)
    grouped = grouped.reshape(TAPS, TAPS, channels, TAPS * channels)
    return jnp.pad(grouped, ((0, 0), (0, 0), (0, 0), (0, channels)))


def summed_part(flat, name_dp, name_space):
    count, slabs = lax.axis_size(name_dp), lax.axis_size(name_space)
    parts = flat.reshape(count, slabs, -1)
    mine = lax.dynamic_index_in_dim(parts, lax.axis_index(name_space), 1, keepdims=False)
    if count != 2:
        return lax.psum_scatter(mine, name_dp, scatter_dimension=0, tiled=True)
    me = lax.axis_index(name_dp)
    kept = lax.dynamic_index_in_dim(mine, me, 0)
    sent = lax.dynamic_index_in_dim(mine, 1 - me, 0)
    return kept + lax.ppermute(sent, name_dp, [(0, 1), (1, 0)])


def body(
    enc_input, dec_input, dec_cotangent, deep_cotangent, enc_weight, dec_weight,
    enc_gain, enc_bias, dec_gain, dec_bias,
):
    _, _, channels, slab_depth, height, width = enc_input.shape
    slabs = lax.axis_size("space")
    depth = slab_depth * slabs
    slab_height = height // slabs
    rows = channels * height
    voxels = depth * height * width
    factor = 1.0 / math.sqrt(lax.axis_size("dp") * voxels)
    me = lax.axis_index("space").reshape(1).astype(jnp.int32)

    def canonical(cells):
        return cells[0, 0].transpose(1, 2, 0, 3).reshape(-1, width)

    enc_pieces = gathered(canonical(enc_input), "space")
    cot_pieces = gathered(canonical(dec_cotangent), "space")
    dec_pieces = gathered(canonical(dec_input), "space")
    deep_pieces = gathered(canonical(deep_cotangent), "space")

    flipped = jnp.swapaxes(dec_weight[0][::-1, :, channels:], 1, 2)
    all_strips = jnp.stack(
        [
            strips(enc_weight[0], channels),
            strips(dec_weight[0][:, :, :channels], channels),
            strips(dec_weight[0][:, :, channels:], channels),
            strips(flipped, channels),
        ]
    )
    shape = jax.ShapeDtypeStruct
    banded = call(
        functools.partial(weights_kernel, channels, height),
        shape((all_strips.shape[0], TAPS * rows, TAPS * rows), BF16),
        [],
        1 << 20,
        "weights",
    )(all_strips)

    def spread(values):
        return jnp.broadcast_to(values[0][:, None], (channels, 128))

    shifted_shape = (depth, TAPS * rows, width)
    cell_shape = (depth, rows, width)
    parts = pltpu.VMEM((depth + 2, TAPS, rows, width), F32)
    padded = pltpu.VMEM((depth + 2, rows + 2 * channels, width), BF16)
    conv_flops = 2 * depth * width * (TAPS * rows) ** 2
    gains, biases = spread(enc_gain), spread(enc_bias)
    enc_shifted, hat, skip, skip_own, scale = call(
        functools.partial(enc_kernel, channels),
        (
            shape(shifted_shape, BF16),
            shape(cell_shape, F32),
            shape(cell_shape, BF16),
            shape((slab_depth, rows, width), BF16),
            shape((channels, 128), F32),
        ),
        [parts, pltpu.VMEM(cell_shape, F32), pltpu.VMEM((2, rows, width), F32)],
        conv_flops,
        "enc",
    )(me, *enc_pieces, banded, gains, biases)
    enc_moved = shifted_2(skip_own, "section", 1)

    skip_grad, cot = call(
        skip_grad_kernel,
        (shape(cell_shape, BF16), shape(cell_shape, BF16)),
        [pltpu.VMEM(shifted_shape, BF16), parts],
        conv_flops,
        "skip_grad",
    )(me, *cot_pieces, banded)

    dec_own, up, down = call(
        functools.partial(dec_kernel, channels),
        (
            shape((depth, slab_height * channels, width), BF16),
            shape(shifted_shape, BF16),
            shape(shifted_shape, BF16),
        ),
        [parts, pltpu.VMEM(cell_shape, F32), pltpu.VMEM((2, rows, width), F32)],
        2 * conv_flops,
        "dec",
    )(me, *dec_pieces, skip, banded, spread(dec_gain), spread(dec_bias))
    dec_moved = shifted_2(dec_own, "section", -1)

    sums = pltpu.VMEM((2, TAPS * TAPS * channels, 128), F32)
    taps = TAPS * TAPS * TAPS
    dec_flat = call(
        functools.partial(dec_grad_kernel, channels, factor),
        shape((taps * channels * 2 * channels // 128, 128), F32),
        [padded, sums],
        conv_flops,
        "dec_grad",
    )(cot, up, down)
    dec_part = summed_part(dec_flat, "dp", "space")

    enc_flat = call(
        functools.partial(enc_grad_kernel, channels, factor),
        shape((taps * channels * channels // 128, 128), F32),
        [pltpu.VMEM(cell_shape, F32), pltpu.VMEM((2, rows, width), F32), padded, pltpu.VMEM((1, TAPS * TAPS * channels, 128), F32)],
        conv_flops,
        "enc_grad",
    )(me, *deep_pieces, skip_grad, hat, scale, gains, biases, enc_shifted)
    enc_part = summed_part(enc_flat, "dp", "space")

    enc_handoff = enc_moved.reshape(slab_depth, height, channels, width).transpose(2, 0, 1, 3)
    dec_handoff = dec_moved.reshape(depth, slab_height, channels, width).transpose(2, 0, 1, 3)
    return (enc_handoff[None, None], dec_handoff[None, None], enc_part.reshape(1, -1), dec_part.reshape(1, -1))


def solution(mesh):
    in_specs = (
        P("section", "dp", None, "space", None, None),
        P("section", "dp", None, None, "space", None),
        P("section", "dp", None, None, "space", None),
        P("section", "dp", None, "space", None, None),
        P("section", None, None, None),
        P("section", None, None, None),
        P("section", None),
        P("section", None),
        P("section", None),
        P("section", None),
    )
    out_specs = (
        P("section", "dp", None, "space", None, None),
        P("section", "dp", None, None, "space", None),
        P("section", ("dp", "space")),
        P("section", ("dp", "space")),
    )
    return jax.shard_map(body, mesh=mesh, in_specs=in_specs, out_specs=out_specs, check_vma=False)
```

```python
import functools
import math

import jax
import jax.numpy as jnp
from jax import lax
from jax.experimental import pallas as pl
from jax.experimental.pallas import tpu as pltpu
from jax.sharding import PartitionSpec as P


EPS = 1e-05
TAPS = 3
PAIR = 2
LIMIT = 12 * 1024 * 1024
BF16 = jnp.bfloat16
F32 = jnp.float32


def call(body, outs, scratch, after=0, in_specs=None, out_specs=None):
    count = len(outs) if isinstance(outs, tuple) else 1

    def kernel(*refs):
        inputs = len(refs) - count - len(scratch)
        body(*refs[: inputs - after], *refs[inputs:])

    specs = {} if in_specs is None else {"in_specs": in_specs}
    specs |= {} if out_specs is None else {"out_specs": out_specs}
    return pl.pallas_call(
        kernel,
        out_shape=outs,
        scratch_shapes=scratch,
        compiler_params=pltpu.CompilerParams(vmem_limit_bytes=LIMIT),
        cost_estimate=pl.CostEstimate(flops=1 << 12, bytes_accessed=1 << 10, transcendentals=0),
        **specs,
    )


def width_shifts(rows):
    width = rows.shape[1]
    lane = lax.broadcasted_iota(jnp.int32, rows.shape, 1)
    none = jnp.zeros_like(rows)
    left = jnp.where(lane == 0, none, pltpu.roll(rows, 1, 1))
    right = jnp.where(lane == width - 1, none, pltpu.roll(rows, width - 1, 1))
    return (left, rows, right)


def row_turn(size, outer, inner):
    shift = inner.bit_length() - 1
    assert 1 << shift == inner and outer * inner == size
    row = lax.broadcasted_iota(jnp.int32, (size, size), 0)
    source = (row & (inner - 1)) * outer + (row >> shift)
    return jnp.where(lax.broadcasted_iota(jnp.int32, (size, size), 1) == source, 1.0, 0.0).astype(BF16)


def prepare_kernel(
    enc_hbm, dec_hbm, g0, g1, g2, g3, own_hbm, cot_hbm, dec_in_hbm, deep_hbm,
    enc_out, flip_out, up_out, down_out, turn_out, back_out, columns_out, own_out, mine_out,
    enc_ref, dec_ref, row0, row1, row2, row3, sems, enc_wide, dec_wide,
):
    size = own_hbm.shape[0]
    rows_of = (row0, row1, row2, row3)
    copies = [
        pltpu.make_async_copy(source, target, sems.at[at])
        for at, (source, target) in enumerate(
            (
                (enc_hbm, enc_ref), (dec_hbm, dec_ref), *zip((g0, g1, g2, g3), rows_of, strict=True),
                (own_hbm, own_out), (cot_hbm, mine_out.at[:size]), (dec_in_hbm, mine_out.at[size : 2 * size]),
                (deep_hbm, mine_out.at[2 * size :]),
            )
        )
    ]
    for copy in copies:
        copy.start()
    channels = enc_ref.shape[1]
    rows = enc_out.shape[0] // TAPS
    lanes = enc_wide.shape[-1]
    lane = lax.broadcasted_iota(jnp.int32, (channels, lanes), 1)
    turn_out[...] = row_turn(turn_out.shape[0], turn_out.shape[0] // channels, channels)
    back_out[...] = row_turn(back_out.shape[0], channels, back_out.shape[0] // channels)
    for copy in copies[:2]:
        copy.wait()
    for wide, source in ((enc_wide, enc_ref), (dec_wide, dec_ref)):
        wide[...] = jnp.zeros_like(wide)
        for tap in range(source.shape[0]):
            wide[tap, :, : source.shape[2]] = source[tap].astype(F32)

    def strip(blocks):
        total = blocks[0]
        for place, block in enumerate(blocks[1:], 1):
            total = total + pltpu.roll(block, place * channels, 1)
        return total

    def first_half(block):
        return jnp.where(lane < channels, block, 0.0)

    def second_half(block):
        return first_half(pltpu.roll(block, lanes - channels, 1))

    def turned(blocks):
        stacked = jnp.concatenate(blocks + [jnp.zeros_like(blocks[0])] * (lanes // channels - TAPS), axis=0)
        return stacked.T[:channels]

    @pl.loop(0, TAPS)
    def _(depth_tap):
        first = pl.multiple_of(depth_tap * rows, rows)
        for width_tap in range(TAPS):
            taps = [TAPS * TAPS * depth_tap + TAPS * b + width_tap for b in range(TAPS)]
            last = dec_wide.shape[0] - 1
            found = (
                (enc_out, strip([enc_wide[tap] for tap in taps])),
                (up_out, strip([first_half(dec_wide[tap]) for tap in taps])),
                (down_out, strip([second_half(dec_wide[tap]) for tap in taps])),
                (flip_out, turned([second_half(dec_wide[last - tap]) for tap in taps])),
            )
            for out_ref, block in found:
                rolled = {}
                for height in range(rows // channels):
                    offset = channels * (height - 1)
                    turn = offset % lanes
                    if turn not in rolled:
                        rolled[turn] = pltpu.roll(block, turn, 1) if turn else block
                    for tile in range(rows // lanes):
                        place = lane + (lanes * tile - offset)
                        inside = (place >= 0) & (place < TAPS * channels)
                        out_ref[
                            pl.ds(first + height * channels, channels),
                            width_tap * rows + tile * lanes : width_tap * rows + (tile + 1) * lanes,
                        ] = jnp.where(inside, rolled[turn], 0.0).astype(BF16)

    for copy in copies[2:]:
        copy.wait()
    for place, row in enumerate(rows_of):
        columns_out[place] = jnp.broadcast_to(column(row), columns_out.shape[1:])


def column(row_ref):
    count = row_ref.shape[1]
    wide = jnp.broadcast_to(row_ref[...], (count, count))
    here = lax.broadcasted_iota(jnp.int32, (count, count), 0) == lax.broadcasted_iota(
        jnp.int32, (count, count), 1
    )
    return jnp.sum(jnp.where(here, wide, 0.0), axis=1, keepdims=True)


def turned_rows(pieces, turn_ref, turned_ref):
    side_by_side = jnp.concatenate([piece[...] for piece in pieces], axis=1)
    turned_ref[...] = jnp.dot(turn_ref[...], side_by_side, preferred_element_type=F32).astype(BF16)


def spread_depth(me, pieces, turn_ref, turned_ref, shifted_ref):
    rows = shifted_ref.shape[1] // TAPS
    width = shifted_ref.shape[2]
    depth = pieces[0].shape[0] // rows
    turned_rows(pieces, turn_ref, turned_ref)
    for distance in range(len(pieces)):
        owner = me ^ distance
        for layer in range(depth):
            cells = turned_ref[layer * rows : (layer + 1) * rows, distance * width : (distance + 1) * width]
            for tap, block in enumerate(width_shifts(cells)):
                shifted_ref[owner * depth + layer, tap * rows : (tap + 1) * rows, :] = block


def spread_height(me, pieces, turn_ref, turned_ref, shifted_ref):
    depth, rows, width = shifted_ref.shape
    rows = rows // TAPS
    part = pieces[0].shape[0] // depth
    turned_rows(pieces, turn_ref, turned_ref)
    for distance in range(len(pieces)):
        owner = me ^ distance
        for layer in range(depth):
            cells = turned_ref[layer * part : (layer + 1) * part, distance * width : (distance + 1) * width]
            for tap, block in enumerate(width_shifts(cells)):
                first = pl.multiple_of(tap * rows + owner * part, part)
                shifted_ref[layer, pl.ds(first, part), :] = block


def taps_product(pairs, parts_ref):
    depth = parts_ref.shape[0] - 2
    rows = parts_ref.shape[2]
    width = parts_ref.shape[3]
    for tap in range(TAPS):
        parts_ref[0, tap] = jnp.zeros((rows, width), F32)
        parts_ref[depth + 1, tap] = jnp.zeros((rows, width), F32)

    @pl.loop(0, depth // 2)
    def _(step):
        total = None
        for weights_ref, shifted_ref in pairs:
            cells = jnp.concatenate([shifted_ref[2 * step], shifted_ref[2 * step + 1]], axis=1)
            product = jnp.dot(weights_ref[...], cells, preferred_element_type=F32)
            total = product if total is None else total + product
        for tap in range(TAPS):
            block = total[tap * rows : (tap + 1) * rows]
            parts_ref[2 * step + 1, tap] = block[:, :width]
            parts_ref[2 * step + 2, tap] = block[:, width:]


def combined(parts_ref, layer):
    total = parts_ref[layer, 0]
    for tap in range(1, TAPS):
        total = total + parts_ref[layer + tap, tap]
    return total


def over_channels(sums, channels):
    total = sums[:channels]
    for first in range(channels, sums.shape[0], channels):
        total = total + sums[first : first + channels]
    return jnp.sum(total, axis=1, keepdims=True)


def tiled(values, count):
    return jnp.concatenate([values] * count, axis=0)


def normalized(parts_ref, pre_ref, sums_ref, channels):
    depth, rows, width = pre_ref.shape
    sums_ref[...] = jnp.zeros_like(sums_ref)

    @pl.loop(0, depth)
    def _(layer):
        pre = combined(parts_ref, layer)
        pre_ref[layer] = pre
        sums_ref[0] += pre
        sums_ref[1] += pre * pre

    cells = depth * (rows // channels) * width
    mean = over_channels(sums_ref[0], channels) * (1.0 / cells)
    square = over_channels(sums_ref[1], channels) * (1.0 / cells)
    return mean, lax.rsqrt(square - mean * mean + EPS)


def enc_kernel(
    channels, me_ref, p0, p1, p2, p3, weights_ref, turn_ref, back_ref, columns_ref,
    shifted_ref, hat_ref, skip_ref, own_ref, scale_ref, turned_ref, parts_ref, pre_ref, sums_ref,
):
    me = me_ref[0]
    depth, rows, _ = pre_ref.shape
    spread_depth(me, (p0, p1, p2, p3), turn_ref, turned_ref, shifted_ref)
    taps_product([(weights_ref, shifted_ref)], parts_ref)
    mean, scale = normalized(parts_ref, pre_ref, sums_ref, channels)
    scale_ref[...] = jnp.broadcast_to(scale, scale_ref.shape)
    count = rows // channels
    means, scales = tiled(mean, count), tiled(scale, count)
    gains, biases = tiled(columns_ref[0, :, :1], count), tiled(columns_ref[1, :, :1], count)

    @pl.loop(0, depth)
    def _(layer):
        hat = (pre_ref[layer] - means) * scales
        hat_ref[layer] = hat
        skip_ref[layer] = jnp.maximum(gains * hat + biases, 0.0).astype(BF16)

    layers = own_ref.shape[0] // rows
    own = jnp.concatenate([skip_ref[me * layers + layer] for layer in range(layers)], axis=0)
    own_ref[...] = jnp.dot(back_ref[...], own, preferred_element_type=F32).astype(BF16)


def piece_views(refs, size, places):
    return [ref.at[place * size : (place + 1) * size] for ref, place in zip(refs, places, strict=True)]


def skip_grad_kernel(
    size, me_ref, p0, p1, p2, p3, weights_ref, turn_ref, grad_ref, cot_ref, shifted_ref, turned_ref, parts_ref
):
    rows = grad_ref.shape[1]
    spread_height(me_ref[0], piece_views((p0, p1, p2, p3), size, (0, 0, 0, 0)), turn_ref, turned_ref, shifted_ref)
    taps_product([(weights_ref, shifted_ref)], parts_ref)

    @pl.loop(0, grad_ref.shape[0])
    def _(layer):
        grad_ref[layer] = combined(parts_ref, layer).astype(BF16)
        cot_ref[layer] = shifted_ref[layer, rows : 2 * rows, :]


def dec_kernel(
    channels, size, me_ref, p0, p1, p2, p3, skip_ref, up_weights_ref, down_weights_ref, turn_ref, back_ref,
    columns_ref, own_ref, up_ref, down_ref, turned_ref, parts_ref, pre_ref, sums_ref,
):
    me = me_ref[0]
    depth, rows, _ = pre_ref.shape
    spread_height(me, piece_views((p0, p1, p2, p3), size, (1, 1, 0, 0)), turn_ref, turned_ref, up_ref)

    for layer in range(depth):
        for tap, block in enumerate(width_shifts(skip_ref[layer])):
            down_ref[layer, tap * rows : (tap + 1) * rows, :] = block

    taps_product([(up_weights_ref, up_ref), (down_weights_ref, down_ref)], parts_ref)
    mean, scale = normalized(parts_ref, pre_ref, sums_ref, channels)
    part = own_ref.shape[0] // depth
    count = part // channels
    means, scales = tiled(mean, count), tiled(scale, count)
    gains, biases = tiled(columns_ref[2, :, :1], count), tiled(columns_ref[3, :, :1], count)

    own = []
    for layer in range(depth):
        pre = pre_ref[layer, pl.ds(pl.multiple_of(me * part, part), part), :]
        hat = (pre - means) * scales
        own.append(jnp.maximum(gains * hat + biases, 0.0).astype(BF16))
    own = jnp.concatenate(own, axis=0)
    own_ref[...] = jnp.dot(back_ref[...], own, preferred_element_type=F32).astype(BF16)


def outer_sums(channels, outers, padded_ref, shifted_refs, sums_ref):
    depth = shifted_refs[0].shape[0]
    rows = shifted_refs[0].shape[1] // TAPS
    lanes = len(shifted_refs) * TAPS * channels

    @pl.loop(0, rows // channels)
    def _(height):
        left = []
        for depth_tap, height_tap in outers:
            first = pl.multiple_of((height + 2 - height_tap) * channels, channels)
            left.append(
                jnp.concatenate(
                    [padded_ref[layer + 2 - depth_tap, pl.ds(first, channels), :] for layer in range(depth)],
                    axis=1,
                )
            )
        right = []
        for width_tap in range(TAPS):
            for shifted_ref in shifted_refs:
                first = pl.multiple_of(width_tap * rows + height * channels, channels)
                right.append(
                    jnp.concatenate(
                        [shifted_ref[layer, pl.ds(first, channels), :] for layer in range(depth)], axis=1
                    )
                )
        product = lax.dot_general(
            jnp.concatenate(left, axis=0),
            jnp.concatenate(right, axis=0),
            (((1,), (1,)), ((), ())),
            preferred_element_type=F32,
        )
        for tile in range(sums_ref.shape[0]):
            block = product[:, tile * 128 : min(lanes, (tile + 1) * 128)]
            old = sums_ref[tile, :, : block.shape[1]]
            sums_ref[tile, :, : block.shape[1]] = jnp.where(height == 0, 0.0, old) + block


def flattened(channels, sources, factor, sums_ref, flat_ref):
    lanes = flat_ref.shape[1]
    span = sources * channels
    merged = lanes // span
    count = channels // merged
    lane = lax.broadcasted_iota(jnp.int32, (count, lanes), 1)
    for outer in range(sums_ref.shape[1] // channels):
        for width_tap in range(TAPS):
            first = width_tap * span
            tile, inner = first // lanes, first % lanes
            total = None
            for row in range(merged):
                block = sums_ref[tile, pl.ds(outer * channels + row, count, stride=merged), :]
                turn = (row * span - inner) % lanes
                block = pltpu.roll(block, turn, 1) if turn else block
                total = block if total is None else jnp.where(lane >= row * span, block, total)
            start = (outer * TAPS + width_tap) * count
            flat_ref[start : start + count, :] = total * factor


def tap_sums(channels, factor, slabs, me_ref, padded_ref, shifted_refs, out_refs, sums_ref, flat_ref):
    blocks = TAPS * TAPS
    if len(out_refs) == 1:
        outers = [(outer // TAPS, outer % TAPS) for outer in range(blocks)]
    else:
        outers, offsets = [], []
        part = out_refs[0].shape[0]
        held = flat_ref.shape[0] // (PAIR * len(out_refs))
        for distance in range(len(out_refs)):
            place = ((me_ref[1] ^ distance) * slabs + me_ref[0]) * part
            first = place // held
            offsets.append(PAIR * distance * held + place - first * held)
            for outer in (first, jnp.minimum(first + 1, blocks - 1)):
                outers.append((outer // TAPS, outer % TAPS))
    outer_sums(channels, outers, padded_ref, shifted_refs, sums_ref)
    flattened(channels, len(shifted_refs), factor, sums_ref, flat_ref)
    if len(out_refs) == 1:
        out_refs[0][...] = flat_ref[...]
    else:
        for out_ref, offset in zip(out_refs, offsets, strict=True):
            out_ref[...] = flat_ref[pl.ds(offset, part), :]


def padded_cells(channels, cells_ref, padded_ref):
    depth, rows, _ = cells_ref.shape
    padded_ref[...] = jnp.zeros_like(padded_ref)

    @pl.loop(0, depth)
    def _(layer):
        padded_ref[layer + 1, channels : channels + rows, :] = cells_ref[layer]


def dec_grad_kernel(channels, factor, slabs, me_ref, cot_ref, up_ref, down_ref, *refs):
    *out_refs, padded_ref, sums_ref, flat_ref = refs
    padded_cells(channels, cot_ref, padded_ref)
    shifted_refs = (up_ref, down_ref)
    tap_sums(channels, factor, slabs, me_ref, padded_ref, shifted_refs, out_refs, sums_ref, flat_ref)


def enc_grad_kernel(
    channels, factor, slabs, me_ref, p0, p1, p2, p3, turn_ref, grad_ref, hat_ref, scale_ref, columns_ref,
    shifted_ref, *refs,
):
    *out_refs, turned_ref, gated_ref, acc_ref, padded_ref, sums_ref, flat_ref = refs
    me = me_ref[0]
    depth, rows, width = hat_ref.shape
    count = rows // channels
    gains, biases = tiled(columns_ref[0, :, :1], count), tiled(columns_ref[1, :, :1], count)
    acc_ref[...] = jnp.zeros_like(acc_ref)
    size = turn_ref.shape[0]
    layers = size // rows
    turned_rows(piece_views((p0, p1, p2, p3), size, (2, 2, 1, 1)), turn_ref, turned_ref)
    for distance in range(turned_ref.shape[1] // width):
        owner = me ^ distance
        piece = turned_ref.at[:, distance * width : (distance + 1) * width]
        for inner in range(layers):
            layer = owner * layers + inner
            hat = hat_ref[layer]
            upstream = grad_ref[layer].astype(F32) + piece[inner * rows : (inner + 1) * rows, :].astype(F32)
            gated = jnp.where(gains * hat + biases > 0, upstream, 0.0) * gains
            gated_ref[layer] = gated
            acc_ref[0] += gated
            acc_ref[1] += gated * hat
    cells = depth * count * width
    first = tiled(over_channels(acc_ref[0], channels) * (1.0 / cells), count)
    second = tiled(over_channels(acc_ref[1], channels) * (1.0 / cells), count)
    scales = tiled(scale_ref[:, :1], count)
    padded_ref[...] = jnp.zeros_like(padded_ref)

    @pl.loop(0, depth)
    def _(layer):
        grad = (gated_ref[layer] - first - hat_ref[layer] * second) * scales
        padded_ref[layer + 1, channels : channels + rows, :] = grad.astype(BF16)

    tap_sums(channels, factor, slabs, me_ref, padded_ref, (shifted_ref,), out_refs, sums_ref, flat_ref)


def swapped(block, distance):
    count = lax.axis_size("space")
    return lax.ppermute(block, "space", [(i, i ^ distance) for i in range(count)])


def shifted_2(block, axis, distance):
    devices = range(lax.axis_size(axis))
    route = [(i - distance, i) for i in devices if i - distance in devices]
    return lax.ppermute(block, axis, route)


def halves(rows):
    count = lax.axis_size("dp") * lax.axis_size("space")
    blocks = TAPS * TAPS
    part, held = rows // count, rows // blocks
    return (
        lax.axis_size("dp") == PAIR
        and rows % count == 0
        and all((place + 1) * part <= (place * part // held + PAIR) * held for place in range(count))
    )


def scattered(flat):
    count, slabs = lax.axis_size("dp"), lax.axis_size("space")
    every = flat.reshape(count, slabs, -1)
    mine = lax.dynamic_index_in_dim(every, lax.axis_index("space"), 1, keepdims=False)
    return lax.psum_scatter(mine, "dp", scatter_dimension=0, tiled=True)


def finish_kernel(sums, *refs):
    moved = refs[:2]
    parts = refs[2 : 2 + 2 * sums]
    *outs, sems = refs[2 + 2 * sums :]
    copies = [
        pltpu.make_async_copy(source, target, sems.at[at])
        for at, (source, target) in enumerate(zip(moved, outs[:2], strict=True))
    ]
    for copy in copies:
        copy.start()
    for at, out in enumerate(outs[2:]):
        kept, received = parts[2 * at : 2 * at + 2]
        total = kept[...] + received[...]
        lanes = total.shape[1]
        for row in range(total.shape[0]):
            out[:, row * lanes : (row + 1) * lanes] = total[row : row + 1]
    for copy in copies:
        copy.wait()


def body(
    enc_input, dec_input, dec_cotangent, deep_cotangent, enc_weight, dec_weight,
    enc_gain, enc_bias, dec_gain, dec_bias,
):
    _, _, channels, slab_depth, height, width = enc_input.shape
    slabs = lax.axis_size("space")
    depth = slab_depth * slabs
    slab_height = height // slabs
    rows = channels * height
    voxels = depth * height * width
    factor = 1.0 / math.sqrt(lax.axis_size("dp") * voxels)
    me = jnp.stack([lax.axis_index("space"), lax.axis_index("dp")]).astype(jnp.int32)

    shape = pltpu.VMEM
    size = channels * slab_depth * height
    far, near = slabs // 2, slabs // 4
    enc_raw, cot_raw, dec_raw, deep_raw = (
        cells.reshape(size, width) for cells in (enc_input, dec_cotangent, dec_input, deep_cotangent)
    )
    enc_far = swapped(enc_raw, far)
    enc_near = swapped(enc_raw, near)
    cot_far = swapped(cot_raw, far)

    square = shape((size, size), BF16)
    matrix = shape((TAPS * rows, TAPS * rows), BF16)
    small = pltpu.VMEM((1, channels), F32)
    wide = pltpu.VMEM((enc_weight.shape[1], channels, 128), F32)
    enc_banded, flip_banded, up_banded, down_banded, turn, back, columns, enc_own, mine = call(
        prepare_kernel,
        (
            matrix, matrix, matrix, matrix, square, square, shape((4, channels, 128), F32),
            shape((size, width), BF16), shape((3 * size, width), BF16),
        ),
        [
            pltpu.VMEM(enc_weight.shape[1:], BF16), pltpu.VMEM(dec_weight.shape[1:], BF16),
            small, small, small, small, pltpu.SemaphoreType.DMA((10,)), wide, wide,
        ],
        1,
        [pl.BlockSpec(memory_space=pltpu.HBM)] * 10 + [pl.BlockSpec(memory_space=pltpu.SMEM)],
    )(
        *(
            pltpu.with_memory_space_constraint(array, pltpu.HBM)
            for array in (
                enc_weight[0], dec_weight[0], enc_gain, enc_bias, dec_gain, dec_bias,
                enc_raw, cot_raw, dec_raw, deep_raw,
            )
        ),
        me,
    )
    others_far = swapped(mine[size:], far)
    others_near = swapped(mine, near)
    enc_relay = swapped(enc_far, near)
    cot_relay = swapped(cot_far, near)
    others_relay = swapped(others_far, near)

    shifted_shape = (depth, TAPS * rows, width)
    cell_shape = (depth, rows, width)
    turned = pltpu.VMEM((size, slabs * width), BF16)
    parts = pltpu.VMEM((depth + 2, TAPS, rows, width), F32)
    padded = pltpu.VMEM((depth + 2, rows + 2 * channels, width), BF16)
    pre, line_sums = pltpu.VMEM(cell_shape, F32), pltpu.VMEM((2, rows, width), F32)
    enc_shifted, hat, skip, skip_own, scale = call(
        functools.partial(enc_kernel, channels),
        (
            shape(shifted_shape, BF16),
            shape(cell_shape, F32),
            shape(cell_shape, BF16),
            shape((size, width), BF16),
            shape((channels, 128), F32),
        ),
        [turned, parts, pre, line_sums],
    )(me, enc_own, enc_near, enc_far, enc_relay, enc_banded, turn, back, columns)
    enc_moved = shifted_2(skip_own, "section", 1)

    skip_grad, cot = call(
        functools.partial(skip_grad_kernel, size),
        (shape(cell_shape, BF16), shape(cell_shape, BF16)),
        [pltpu.VMEM(shifted_shape, BF16), turned, parts],
        1,
    )(me, mine, others_near, cot_far, cot_relay, flip_banded, turn, scale)

    dec_act, up, down = call(
        functools.partial(dec_kernel, channels, size),
        (shape((size, width), BF16), shape(shifted_shape, BF16), shape(shifted_shape, BF16)),
        [turned, parts, pre, line_sums],
        1,
    )(
        me, mine, others_near, others_far, others_relay, skip, up_banded, down_banded, turn, back, columns,
        skip_grad,
    )
    dec_moved = shifted_2(dec_act, "section", -1)

    flat_rows = TAPS * TAPS * TAPS * channels * channels // 128
    pair = halves(flat_rows) and halves(2 * flat_rows)

    def grad_shapes(total):
        if not pair:
            return (shape((total, 128), F32),)
        return (shape((total // (PAIR * slabs), 128), F32),) * 2

    def grad_scratch(total, tiles):
        outers = 2 * PAIR if pair else TAPS * TAPS
        held = total // (TAPS * TAPS) * outers
        return [padded, pltpu.VMEM((tiles, outers * channels, 128), F32), pltpu.VMEM((held, 128), F32)]

    dec_flat = call(
        functools.partial(dec_grad_kernel, channels, factor, slabs),
        grad_shapes(2 * flat_rows),
        grad_scratch(2 * flat_rows, 2),
    )(me, cot, up, down)
    enc_flat = call(
        functools.partial(enc_grad_kernel, channels, factor, slabs),
        grad_shapes(flat_rows),
        [turned, pre, line_sums, *grad_scratch(flat_rows, 1)],
        1,
    )(
        me, mine, others_near, others_far, others_relay, turn, skip_grad, hat, scale, columns, enc_shifted,
        dec_flat[0],
    )

    operands, sums, ends = [enc_moved, dec_moved], 0, []
    if pair:
        for (kept, sent) in (enc_flat, dec_flat):
            operands += [kept, lax.ppermute(sent, "dp", [(0, 1), (1, 0)])]
            ends.append(jax.ShapeDtypeStruct((1, kept.size), F32))
            sums += 1
    moved = jax.ShapeDtypeStruct((size, width), BF16)
    enc_handoff, dec_handoff, *grads = call(
        functools.partial(finish_kernel, sums),
        (moved, moved, *ends),
        [pltpu.SemaphoreType.DMA((2,))],
        0,
        None,
        (pl.BlockSpec(memory_space=pl.ANY),) * 2 + (pl.BlockSpec(memory_space=pltpu.VMEM),) * sums,
    )(*operands)
    if not pair:
        grads = [scattered(enc_flat[0]), scattered(dec_flat[0])]
    enc_handoff = enc_handoff.reshape(1, 1, channels, slab_depth, height, width)
    dec_handoff = dec_handoff.reshape(1, 1, channels, depth, slab_height, width)
    return (enc_handoff, dec_handoff, grads[0].reshape(1, -1), grads[1].reshape(1, -1))


def solution(mesh):
    in_specs = (
        P("section", "dp", None, "space", None, None),
        P("section", "dp", None, None, "space", None),
        P("section", "dp", None, None, "space", None),
        P("section", "dp", None, "space", None, None),
        P("section", None, None, None),
        P("section", None, None, None),
        P("section", None),
        P("section", None),
        P("section", None),
        P("section", None),
    )
    out_specs = (
        P("section", "dp", None, "space", None, None),
        P("section", "dp", None, None, "space", None),
        P("section", ("dp", "space")),
        P("section", ("dp", "space")),
    )

    return jax.shard_map(body, mesh=mesh, in_specs=in_specs, out_specs=out_specs, check_vma=False)
```

```python
import functools
import math

import jax
import jax.numpy as jnp
from jax import lax
from jax.experimental import pallas as pl
from jax.experimental.pallas import tpu as pltpu
from jax.sharding import PartitionSpec as P


EPS = 1e-05
TAPS = 3
PAIR = 2
LIMIT = 12 * 1024 * 1024
BF16 = jnp.bfloat16
F32 = jnp.float32


def call(body, outs, scratch, after=0, in_specs=None, out_specs=None):
    count = len(outs) if isinstance(outs, tuple) else 1

    def kernel(*refs):
        inputs = len(refs) - count - len(scratch)
        body(*refs[: inputs - after], *refs[inputs:])

    specs = {} if in_specs is None else {"in_specs": in_specs}
    specs |= {} if out_specs is None else {"out_specs": out_specs}
    return pl.pallas_call(
        kernel,
        out_shape=outs,
        scratch_shapes=scratch,
        compiler_params=pltpu.CompilerParams(vmem_limit_bytes=LIMIT),
        cost_estimate=pl.CostEstimate(flops=1 << 12, bytes_accessed=1 << 10, transcendentals=0),
        **specs,
    )


def width_shifts(rows):
    width = rows.shape[1]
    lane = lax.broadcasted_iota(jnp.int32, rows.shape, 1)
    none = jnp.zeros_like(rows)
    left = jnp.where(lane == 0, none, pltpu.roll(rows, 1, 1))
    right = jnp.where(lane == width - 1, none, pltpu.roll(rows, width - 1, 1))
    return (left, rows, right)


def row_turn(size, outer, inner):
    shift = inner.bit_length() - 1
    assert 1 << shift == inner and outer * inner == size
    row = lax.broadcasted_iota(jnp.int32, (size, size), 0)
    source = (row & (inner - 1)) * outer + (row >> shift)
    return jnp.where(lax.broadcasted_iota(jnp.int32, (size, size), 1) == source, 1.0, 0.0).astype(BF16)


def banded(first, width_tap, found, lane):
    channels, lanes = lane.shape
    for out_ref, block in found:
        rows = out_ref.shape[0] // TAPS
        rolled = {}
        for height in range(rows // channels):
            offset = channels * (height - 1)
            turn = offset % lanes
            if turn not in rolled:
                rolled[turn] = pltpu.roll(block, turn, 1) if turn else block
            for tile in range(rows // lanes):
                place = lane + (lanes * tile - offset)
                inside = (place >= 0) & (place < TAPS * channels)
                out_ref[
                    pl.ds(first + height * channels, channels),
                    width_tap * rows + tile * lanes : width_tap * rows + (tile + 1) * lanes,
                ] = jnp.where(inside, rolled[turn], 0.0).astype(BF16)


def strip(blocks):
    total = blocks[0]
    for place, block in enumerate(blocks[1:], 1):
        total = total + pltpu.roll(block, place * block.shape[0], 1)
    return total


def widened(source, wide):
    wide[...] = jnp.zeros_like(wide)
    for tap in range(source.shape[0]):
        wide[tap, :, : source.shape[2]] = source[tap].astype(F32)


def height_taps(depth_tap, width_tap):
    return [TAPS * TAPS * depth_tap + TAPS * height_tap + width_tap for height_tap in range(TAPS)]


def prepare_kernel(
    enc_hbm, dec_hbm, g0, g1, g2, g3, own_hbm, cot_hbm, dec_in_hbm, deep_hbm,
    enc_out, turn_out, back_out, columns_out, own_out, mine_out, dec_ref,
    enc_ref, row0, row1, row2, row3, sems, enc_wide,
):
    size = own_hbm.shape[0]
    channels = enc_ref.shape[1]
    rows_of = (row0, row1, row2, row3)
    copies = [
        pltpu.make_async_copy(source, target, sems.at[at])
        for at, (source, target) in enumerate(
            (
                (enc_hbm, enc_ref), (dec_hbm, dec_ref), *zip((g0, g1, g2, g3), rows_of, strict=True),
                (own_hbm, own_out), (cot_hbm, mine_out.at[:size]), (dec_in_hbm, mine_out.at[size : 2 * size]),
                (deep_hbm, mine_out.at[2 * size :]),
            )
        )
    ]
    for copy in copies:
        copy.start()
    lane = lax.broadcasted_iota(jnp.int32, (channels, enc_wide.shape[-1]), 1)
    turn_out[...] = row_turn(turn_out.shape[0], turn_out.shape[0] // channels, channels)
    back_out[...] = row_turn(back_out.shape[0], channels, back_out.shape[0] // channels)
    copies[0].wait()
    widened(enc_ref, enc_wide)

    @pl.loop(0, TAPS)
    def _(depth_tap):
        first = pl.multiple_of(depth_tap * (enc_out.shape[0] // TAPS), enc_out.shape[0] // TAPS)
        for width_tap in range(TAPS):
            taps = height_taps(depth_tap, width_tap)
            banded(first, width_tap, [(enc_out, strip([enc_wide[tap] for tap in taps]))], lane)

    for copy in copies[1:]:
        copy.wait()
    for place, row in enumerate(rows_of):
        columns_out[place] = jnp.broadcast_to(column(row), columns_out.shape[1:])


def weights_kernel(dec_ref, flip_out, up_out, down_out, wide):
    channels = dec_ref.shape[1]
    lanes = wide.shape[-1]
    lane = lax.broadcasted_iota(jnp.int32, (channels, lanes), 1)
    last = dec_ref.shape[0] - 1
    widened(dec_ref, wide)

    def first_half(block):
        return jnp.where(lane < channels, block, 0.0)

    def second_half(block):
        return first_half(pltpu.roll(block, lanes - channels, 1))

    def turned(blocks):
        stacked = jnp.concatenate(blocks + [jnp.zeros_like(blocks[0])] * (lanes // channels - TAPS), axis=0)
        return stacked.T[:channels]

    @pl.loop(0, TAPS)
    def _(depth_tap):
        first = pl.multiple_of(depth_tap * (flip_out.shape[0] // TAPS), flip_out.shape[0] // TAPS)
        for width_tap in range(TAPS):
            taps = height_taps(depth_tap, width_tap)
            found = [
                (up_out, strip([first_half(wide[tap]) for tap in taps])),
                (down_out, strip([second_half(wide[tap]) for tap in taps])),
                (flip_out, turned([second_half(wide[last - tap]) for tap in taps])),
            ]
            banded(first, width_tap, found, lane)


def column(row_ref):
    count = row_ref.shape[1]
    wide = jnp.broadcast_to(row_ref[...], (count, count))
    here = lax.broadcasted_iota(jnp.int32, (count, count), 0) == lax.broadcasted_iota(
        jnp.int32, (count, count), 1
    )
    return jnp.sum(jnp.where(here, wide, 0.0), axis=1, keepdims=True)


def turned_rows(pieces, turn_ref, turned_ref):
    side_by_side = jnp.concatenate([piece[...] for piece in pieces], axis=1)
    turned_ref[...] = jnp.dot(turn_ref[...], side_by_side, preferred_element_type=F32).astype(BF16)


def spread_depth(me, pieces, turn_ref, turned_ref, shifted_ref):
    rows = shifted_ref.shape[1] // TAPS
    width = shifted_ref.shape[2]
    depth = pieces[0].shape[0] // rows
    turned_rows(pieces, turn_ref, turned_ref)
    for distance in range(len(pieces)):
        owner = me ^ distance
        for layer in range(depth):
            cells = turned_ref[layer * rows : (layer + 1) * rows, distance * width : (distance + 1) * width]
            for tap, block in enumerate(width_shifts(cells)):
                shifted_ref[owner * depth + layer, tap * rows : (tap + 1) * rows, :] = block


def spread_height(me, pieces, turn_ref, turned_ref, shifted_ref):
    depth, rows, width = shifted_ref.shape
    rows = rows // TAPS
    part = pieces[0].shape[0] // depth
    turned_rows(pieces, turn_ref, turned_ref)
    for distance in range(len(pieces)):
        owner = me ^ distance
        for layer in range(depth):
            cells = turned_ref[layer * part : (layer + 1) * part, distance * width : (distance + 1) * width]
            for tap, block in enumerate(width_shifts(cells)):
                first = pl.multiple_of(tap * rows + owner * part, part)
                shifted_ref[layer, pl.ds(first, part), :] = block


def taps_product(pairs, parts_ref):
    depth = parts_ref.shape[0] - 2
    rows = parts_ref.shape[2]
    width = parts_ref.shape[3]
    for tap in range(TAPS):
        parts_ref[0, tap] = jnp.zeros((rows, width), F32)
        parts_ref[depth + 1, tap] = jnp.zeros((rows, width), F32)

    @pl.loop(0, depth // 2)
    def _(step):
        total = None
        for weights_ref, shifted_ref in pairs:
            cells = jnp.concatenate([shifted_ref[2 * step], shifted_ref[2 * step + 1]], axis=1)
            product = jnp.dot(weights_ref[...], cells, preferred_element_type=F32)
            total = product if total is None else total + product
        for tap in range(TAPS):
            block = total[tap * rows : (tap + 1) * rows]
            parts_ref[2 * step + 1, tap] = block[:, :width]
            parts_ref[2 * step + 2, tap] = block[:, width:]


def combined(parts_ref, layer):
    total = parts_ref[layer, 0]
    for tap in range(1, TAPS):
        total = total + parts_ref[layer + tap, tap]
    return total


def over_channels(sums, channels):
    total = sums[:channels]
    for first in range(channels, sums.shape[0], channels):
        total = total + sums[first : first + channels]
    return jnp.sum(total, axis=1, keepdims=True)


def tiled(values, count):
    return jnp.concatenate([values] * count, axis=0)


def normalized(parts_ref, pre_ref, sums_ref, channels):
    depth, rows, width = pre_ref.shape
    sums_ref[...] = jnp.zeros_like(sums_ref)

    @pl.loop(0, depth)
    def _(layer):
        pre = combined(parts_ref, layer)
        pre_ref[layer] = pre
        sums_ref[0] += pre
        sums_ref[1] += pre * pre

    cells = depth * (rows // channels) * width
    mean = over_channels(sums_ref[0], channels) * (1.0 / cells)
    square = over_channels(sums_ref[1], channels) * (1.0 / cells)
    return mean, lax.rsqrt(square - mean * mean + EPS)


def enc_kernel(
    channels, me_ref, p0, p1, p2, p3, weights_ref, turn_ref, back_ref, columns_ref,
    shifted_ref, hat_ref, skip_ref, own_ref, scale_ref, turned_ref, parts_ref, pre_ref, sums_ref,
):
    me = me_ref[0]
    depth, rows, _ = pre_ref.shape
    spread_depth(me, (p0, p1, p2, p3), turn_ref, turned_ref, shifted_ref)
    taps_product([(weights_ref, shifted_ref)], parts_ref)
    mean, scale = normalized(parts_ref, pre_ref, sums_ref, channels)
    scale_ref[...] = jnp.broadcast_to(scale, scale_ref.shape)
    count = rows // channels
    means, scales = tiled(mean, count), tiled(scale, count)
    gains, biases = tiled(columns_ref[0, :, :1], count), tiled(columns_ref[1, :, :1], count)

    @pl.loop(0, depth)
    def _(layer):
        hat = (pre_ref[layer] - means) * scales
        hat_ref[layer] = hat
        skip_ref[layer] = jnp.maximum(gains * hat + biases, 0.0).astype(BF16)

    layers = own_ref.shape[0] // rows
    own = jnp.concatenate([skip_ref[me * layers + layer] for layer in range(layers)], axis=0)
    own_ref[...] = jnp.dot(back_ref[...], own, preferred_element_type=F32).astype(BF16)


def piece_views(refs, size, places):
    return [ref.at[place * size : (place + 1) * size] for ref, place in zip(refs, places, strict=True)]


def skip_grad_kernel(
    size, me_ref, p0, p1, p2, p3, weights_ref, turn_ref, grad_ref, cot_ref, shifted_ref, turned_ref, parts_ref
):
    rows = grad_ref.shape[1]
    spread_height(me_ref[0], piece_views((p0, p1, p2, p3), size, (0, 0, 0, 0)), turn_ref, turned_ref, shifted_ref)
    taps_product([(weights_ref, shifted_ref)], parts_ref)

    @pl.loop(0, grad_ref.shape[0])
    def _(layer):
        grad_ref[layer] = combined(parts_ref, layer).astype(BF16)
        cot_ref[layer] = shifted_ref[layer, rows : 2 * rows, :]


def dec_kernel(
    channels, size, me_ref, p0, p1, p2, p3, skip_ref, up_weights_ref, down_weights_ref, turn_ref, back_ref,
    columns_ref, skip_own_ref, first_ref, second_ref, up_ref, down_ref, turned_ref, parts_ref, pre_ref, sums_ref,
):
    me = me_ref[0]
    depth, rows, _ = pre_ref.shape
    spread_height(me, piece_views((p0, p1, p2, p3), size, (1, 1, 0, 0)), turn_ref, turned_ref, up_ref)

    for layer in range(depth):
        for tap, block in enumerate(width_shifts(skip_ref[layer])):
            down_ref[layer, tap * rows : (tap + 1) * rows, :] = block

    taps_product([(up_weights_ref, up_ref), (down_weights_ref, down_ref)], parts_ref)
    mean, scale = normalized(parts_ref, pre_ref, sums_ref, channels)
    part = size // depth
    count = part // channels
    means, scales = tiled(mean, count), tiled(scale, count)
    gains, biases = tiled(columns_ref[2, :, :1], count), tiled(columns_ref[3, :, :1], count)

    own = []
    for layer in range(depth):
        pre = pre_ref[layer, pl.ds(pl.multiple_of(me * part, part), part), :]
        hat = (pre - means) * scales
        own.append(jnp.maximum(gains * hat + biases, 0.0).astype(BF16))
    own = jnp.concatenate(own, axis=0)
    own = jnp.dot(back_ref[...], own, preferred_element_type=F32).astype(BF16)
    even = (me_ref[2] & 1) == 0

    @pl.when(even)
    def _():
        first_ref[...] = skip_own_ref[...]
        second_ref[...] = own

    @pl.when(jnp.logical_not(even))
    def _():
        first_ref[...] = own
        second_ref[...] = skip_own_ref[...]


def outer_sums(channels, outers, padded_ref, shifted_refs, sums_ref):
    depth = shifted_refs[0].shape[0]
    rows = shifted_refs[0].shape[1] // TAPS
    lanes = len(shifted_refs) * TAPS * channels

    @pl.loop(0, rows // channels)
    def _(height):
        left = []
        for depth_tap, height_tap in outers:
            first = pl.multiple_of((height + 2 - height_tap) * channels, channels)
            left.append(
                jnp.concatenate(
                    [padded_ref[layer + 2 - depth_tap, pl.ds(first, channels), :] for layer in range(depth)],
                    axis=1,
                )
            )
        right = []
        for width_tap in range(TAPS):
            for shifted_ref in shifted_refs:
                first = pl.multiple_of(width_tap * rows + height * channels, channels)
                right.append(
                    jnp.concatenate(
                        [shifted_ref[layer, pl.ds(first, channels), :] for layer in range(depth)], axis=1
                    )
                )
        product = lax.dot_general(
            jnp.concatenate(left, axis=0),
            jnp.concatenate(right, axis=0),
            (((1,), (1,)), ((), ())),
            preferred_element_type=F32,
        )
        for tile in range(sums_ref.shape[0]):
            block = product[:, tile * 128 : min(lanes, (tile + 1) * 128)]
            old = sums_ref[tile, :, : block.shape[1]]
            sums_ref[tile, :, : block.shape[1]] = jnp.where(height == 0, 0.0, old) + block


def flattened(channels, sources, factor, sums_ref, flat_ref):
    lanes = flat_ref.shape[1]
    span = sources * channels
    merged = lanes // span
    count = channels // merged
    lane = lax.broadcasted_iota(jnp.int32, (count, lanes), 1)
    for outer in range(sums_ref.shape[1] // channels):
        for width_tap in range(TAPS):
            first = width_tap * span
            tile, inner = first // lanes, first % lanes
            total = None
            for row in range(merged):
                block = sums_ref[tile, pl.ds(outer * channels + row, count, stride=merged), :]
                turn = (row * span - inner) % lanes
                block = pltpu.roll(block, turn, 1) if turn else block
                total = block if total is None else jnp.where(lane >= row * span, block, total)
            start = (outer * TAPS + width_tap) * count
            flat_ref[start : start + count, :] = total * factor


def tap_sums(channels, factor, slabs, me_ref, padded_ref, shifted_refs, out_refs, sums_ref, flat_ref):
    blocks = TAPS * TAPS
    if len(out_refs) == 1:
        outers = [(outer // TAPS, outer % TAPS) for outer in range(blocks)]
    else:
        outers, offsets = [], []
        part = out_refs[0].shape[0]
        held = flat_ref.shape[0] // (PAIR * len(out_refs))
        for distance in range(len(out_refs)):
            place = ((me_ref[1] ^ distance) * slabs + me_ref[0]) * part
            first = place // held
            offsets.append(PAIR * distance * held + place - first * held)
            for outer in (first, jnp.minimum(first + 1, blocks - 1)):
                outers.append((outer // TAPS, outer % TAPS))
    outer_sums(channels, outers, padded_ref, shifted_refs, sums_ref)
    flattened(channels, len(shifted_refs), factor, sums_ref, flat_ref)
    if len(out_refs) == 1:
        out_refs[0][...] = flat_ref[...]
    else:
        for out_ref, offset in zip(out_refs, offsets, strict=True):
            out_ref[...] = flat_ref[pl.ds(offset, part), :]


def padded_cells(channels, cells_ref, padded_ref):
    depth, rows, _ = cells_ref.shape
    padded_ref[...] = jnp.zeros_like(padded_ref)

    @pl.loop(0, depth)
    def _(layer):
        padded_ref[layer + 1, channels : channels + rows, :] = cells_ref[layer]


def dec_grad_kernel(channels, factor, slabs, me_ref, cot_ref, up_ref, down_ref, *refs):
    *out_refs, padded_ref, sums_ref, flat_ref = refs
    padded_cells(channels, cot_ref, padded_ref)
    shifted_refs = (up_ref, down_ref)
    tap_sums(channels, factor, slabs, me_ref, padded_ref, shifted_refs, out_refs, sums_ref, flat_ref)


def enc_grad_kernel(
    channels, factor, slabs, me_ref, p0, p1, p2, p3, turn_ref, grad_ref, hat_ref, scale_ref, columns_ref,
    shifted_ref, *refs,
):
    *out_refs, turned_ref, gated_ref, acc_ref, padded_ref, sums_ref, flat_ref = refs
    dec_refs = []
    if len(out_refs) > 1:
        dec_refs, out_refs = out_refs[:PAIR], out_refs[PAIR:]
    me = me_ref[0]
    depth, rows, width = hat_ref.shape
    count = rows // channels
    gains, biases = tiled(columns_ref[0, :, :1], count), tiled(columns_ref[1, :, :1], count)
    acc_ref[...] = jnp.zeros_like(acc_ref)
    size = turn_ref.shape[0]
    layers = size // rows
    turned_rows(piece_views((p0, p1, p2, p3), size, (2, 2, 1, 1)), turn_ref, turned_ref)
    for distance in range(turned_ref.shape[1] // width):
        owner = me ^ distance
        piece = turned_ref.at[:, distance * width : (distance + 1) * width]
        for inner in range(layers):
            layer = owner * layers + inner
            hat = hat_ref[layer]
            upstream = grad_ref[layer].astype(F32) + piece[inner * rows : (inner + 1) * rows, :].astype(F32)
            gated = jnp.where(gains * hat + biases > 0, upstream, 0.0) * gains
            gated_ref[layer] = gated
            acc_ref[0] += gated
            acc_ref[1] += gated * hat
    cells = depth * count * width
    first = tiled(over_channels(acc_ref[0], channels) * (1.0 / cells), count)
    second = tiled(over_channels(acc_ref[1], channels) * (1.0 / cells), count)
    scales = tiled(scale_ref[:, :1], count)
    padded_ref[...] = jnp.zeros_like(padded_ref)

    @pl.loop(0, depth)
    def _(layer):
        grad = (gated_ref[layer] - first - hat_ref[layer] * second) * scales
        padded_ref[layer + 1, channels : channels + rows, :] = grad.astype(BF16)

    own_refs = list(out_refs)
    for at, dec_ref in enumerate(dec_refs):
        count = dec_ref.shape[0]
        out_refs[at][:count, :] = dec_ref[...]
        own_refs[at] = out_refs[at].at[count:]
    tap_sums(channels, factor, slabs, me_ref, padded_ref, (shifted_ref,), own_refs, sums_ref, flat_ref)


def swapped(block, distance):
    count = lax.axis_size("space")
    return lax.ppermute(block, "space", [(i, i ^ distance) for i in range(count)])


def paired(block, start):
    count, copies = lax.axis_size("section"), lax.axis_size("dp")
    route = []
    for section in range(count):
        upper = (section - start) % 2
        partner = section - 1 if upper else section + 1
        for copy in range(copies):
            to = (partner, copy) if start <= min(section, partner) and partner < count else (section, copy ^ 1)
            if to[1] < copies:
                route.append((section * copies + copy, to[0] * copies + to[1]))
    return lax.ppermute(block, ("section", "dp"), route)


def halves(rows):
    count = lax.axis_size("dp") * lax.axis_size("space")
    blocks = TAPS * TAPS
    part, held = rows // count, rows // blocks
    return (
        lax.axis_size("dp") == PAIR
        and rows % count == 0
        and all((place + 1) * part <= (place * part // held + PAIR) * held for place in range(count))
    )


def scattered(flat):
    count, slabs = lax.axis_size("dp"), lax.axis_size("space")
    every = flat.reshape(count, slabs, -1)
    mine = lax.dynamic_index_in_dim(every, lax.axis_index("space"), 1, keepdims=False)
    return lax.psum_scatter(mine, "dp", scatter_dimension=0, tiled=True)


def put_kernel(sections, me_ref, first_ref, second_ref, enc_out, dec_out, none_ref, sems):
    none_ref[...] = jnp.zeros_like(none_ref)
    section = me_ref[2]
    last = section == sections - 1
    even = (section & 1) == 0

    def put(case, enc_from, dec_from):
        @pl.when(case)
        def _():
            copies = (
                pltpu.make_async_copy(enc_from, enc_out, sems.at[0]),
                pltpu.make_async_copy(dec_from, dec_out, sems.at[1]),
            )
            for copy in copies:
                copy.start()
            for copy in copies:
                copy.wait()

    inner = (section > 0) & jnp.logical_not(last)
    put((section == 0) & jnp.logical_not(last), none_ref, first_ref)
    put(inner & even, second_ref, first_ref)
    put(inner & jnp.logical_not(even), first_ref, second_ref)
    put(last & even & (section > 0), second_ref, none_ref)
    put(last & jnp.logical_not(even), first_ref, none_ref)
    put(last & (section == 0), none_ref, none_ref)


def finish_kernel(kept_ref, received_ref, *outs):
    first = 0
    for out in outs:
        lanes = kept_ref.shape[1]
        count = out.shape[1] // lanes
        total = kept_ref[first : first + count, :] + received_ref[first : first + count, :]
        for row in range(count):
            out[:, row * lanes : (row + 1) * lanes] = total[row : row + 1]
        first += count


def body(
    enc_input, dec_input, dec_cotangent, deep_cotangent, enc_weight, dec_weight,
    enc_gain, enc_bias, dec_gain, dec_bias,
):
    _, _, channels, slab_depth, height, width = enc_input.shape
    slabs = lax.axis_size("space")
    depth = slab_depth * slabs
    slab_height = height // slabs
    rows = channels * height
    voxels = depth * height * width
    factor = 1.0 / math.sqrt(lax.axis_size("dp") * voxels)
    me = jnp.stack([lax.axis_index("space"), lax.axis_index("dp"), lax.axis_index("section")]).astype(jnp.int32)

    shape = pltpu.VMEM
    size = channels * slab_depth * height
    far, near = slabs // 2, slabs // 4
    enc_raw, cot_raw, dec_raw, deep_raw = (
        cells.reshape(size, width) for cells in (enc_input, dec_cotangent, dec_input, deep_cotangent)
    )
    enc_far = swapped(enc_raw, far)
    enc_near = swapped(enc_raw, near)
    cot_far = swapped(cot_raw, far)

    square = shape((size, size), BF16)
    matrix = shape((TAPS * rows, TAPS * rows), BF16)
    small = pltpu.VMEM((1, channels), F32)
    wide = pltpu.VMEM((enc_weight.shape[1], channels, 128), F32)
    enc_banded, turn, back, columns, enc_own, mine, dec_taps = call(
        prepare_kernel,
        (
            matrix, square, square, shape((4, channels, 128), F32), shape((size, width), BF16),
            shape((3 * size, width), BF16), shape(dec_weight.shape[1:], BF16),
        ),
        [
            pltpu.VMEM(enc_weight.shape[1:], BF16), small, small, small, small,
            pltpu.SemaphoreType.DMA((10,)), wide,
        ],
        1,
        [pl.BlockSpec(memory_space=pltpu.HBM)] * 10 + [pl.BlockSpec(memory_space=pltpu.SMEM)],
    )(
        *(
            pltpu.with_memory_space_constraint(array, pltpu.HBM)
            for array in (
                enc_weight[0], dec_weight[0], enc_gain, enc_bias, dec_gain, dec_bias,
                enc_raw, cot_raw, dec_raw, deep_raw,
            )
        ),
        me,
    )
    others_far = swapped(mine[size:], far)
    others_near = swapped(mine, near)
    enc_relay = swapped(enc_far, near)
    cot_relay = swapped(cot_far, near)
    others_relay = swapped(others_far, near)

    shifted_shape = (depth, TAPS * rows, width)
    cell_shape = (depth, rows, width)
    turned = pltpu.VMEM((size, slabs * width), BF16)
    parts = pltpu.VMEM((depth + 2, TAPS, rows, width), F32)
    padded = pltpu.VMEM((depth + 2, rows + 2 * channels, width), BF16)
    pre, line_sums = pltpu.VMEM(cell_shape, F32), pltpu.VMEM((2, rows, width), F32)
    enc_shifted, hat, skip, skip_own, scale = call(
        functools.partial(enc_kernel, channels),
        (
            shape(shifted_shape, BF16),
            shape(cell_shape, F32),
            shape(cell_shape, BF16),
            shape((size, width), BF16),
            shape((channels, 128), F32),
        ),
        [turned, parts, pre, line_sums],
    )(me, enc_own, enc_near, enc_far, enc_relay, enc_banded, turn, back, columns)
    flip_banded, up_banded, down_banded = call(weights_kernel, (matrix, matrix, matrix), [wide], 1)(dec_taps, scale)

    skip_grad, cot = call(
        functools.partial(skip_grad_kernel, size),
        (shape(cell_shape, BF16), shape(cell_shape, BF16)),
        [pltpu.VMEM(shifted_shape, BF16), turned, parts],
        1,
    )(me, mine, others_near, cot_far, cot_relay, flip_banded, turn, scale)

    first, second, up, down = call(
        functools.partial(dec_kernel, channels, size),
        (shape((size, width), BF16),) * 2 + (shape(shifted_shape, BF16),) * 2,
        [turned, parts, pre, line_sums],
        1,
    )(
        me, mine, others_near, others_far, others_relay, skip, up_banded, down_banded, turn, back, columns,
        skip_own, skip_grad,
    )
    first = paired(first, 0)

    flat_rows = TAPS * TAPS * TAPS * channels * channels // 128
    pair = halves(flat_rows) and halves(2 * flat_rows)

    def grad_shapes(total):
        if not pair:
            return (shape((total, 128), F32),)
        return (shape((total // (PAIR * slabs), 128), F32),) * 2

    def grad_scratch(total, tiles):
        outers = 2 * PAIR if pair else TAPS * TAPS
        held = total // (TAPS * TAPS) * outers
        return [padded, pltpu.VMEM((tiles, outers * channels, 128), F32), pltpu.VMEM((held, 128), F32)]

    dec_flat = call(
        functools.partial(dec_grad_kernel, channels, factor, slabs),
        grad_shapes(2 * flat_rows),
        grad_scratch(2 * flat_rows, 2),
    )(me, cot, up, down)
    second = paired(lax.optimization_barrier((second, dec_flat[0]))[0], 1)
    enc_flat = call(
        functools.partial(enc_grad_kernel, channels, factor, slabs),
        tuple(shape((3 * flat_rows // (PAIR * slabs), 128), F32) for _ in range(PAIR))
        if pair
        else grad_shapes(flat_rows),
        [turned, pre, line_sums, *grad_scratch(flat_rows, 1)],
        0 if pair else 1,
    )(
        me, mine, others_near, others_far, others_relay, turn, skip_grad, hat, scale, columns, enc_shifted,
        *dec_flat,
    )

    moved = jax.ShapeDtypeStruct((size, width), BF16)
    enc_handoff, dec_handoff = call(
        functools.partial(put_kernel, lax.axis_size("section")),
        (moved, moved),
        [pltpu.VMEM((size, width), BF16), pltpu.SemaphoreType.DMA((2,))],
        1,
        None,
        (pl.BlockSpec(memory_space=pl.ANY),) * 2,
    )(me, first, second, enc_flat[0])
    if pair:
        kept, sent = enc_flat
        received = lax.ppermute(sent, "dp", [(0, 1), (1, 0)])
        ends = tuple(
            jax.ShapeDtypeStruct((1, rows * 128), F32)
            for rows in (dec_flat[0].shape[0], kept.shape[0] - dec_flat[0].shape[0])
        )
        grads = call(finish_kernel, ends, [])(kept, received)
    else:
        grads = [scattered(dec_flat[0]), scattered(enc_flat[0])]
    enc_handoff = enc_handoff.reshape(1, 1, channels, slab_depth, height, width)
    dec_handoff = dec_handoff.reshape(1, 1, channels, depth, slab_height, width)
    return (enc_handoff, dec_handoff, grads[1].reshape(1, -1), grads[0].reshape(1, -1))


def solution(mesh):
    in_specs = (
        P("section", "dp", None, "space", None, None),
        P("section", "dp", None, None, "space", None),
        P("section", "dp", None, None, "space", None),
        P("section", "dp", None, "space", None, None),
        P("section", None, None, None),
        P("section", None, None, None),
        P("section", None),
        P("section", None),
        P("section", None),
        P("section", None),
    )
    out_specs = (
        P("section", "dp", None, "space", None, None),
        P("section", "dp", None, None, "space", None),
        P("section", ("dp", "space")),
        P("section", ("dp", "space")),
    )

    return jax.shard_map(body, mesh=mesh, in_specs=in_specs, out_specs=out_specs, check_vma=False)
```

```python
import functools
import math

import jax
import jax.numpy as jnp
from jax import lax
from jax.experimental import pallas as pl
from jax.experimental.pallas import tpu as pltpu
from jax.sharding import PartitionSpec as P


EPS = 1e-05
TAPS = 3
PAIR = 2
ROWS = 16
LIMIT = 12 * 1024 * 1024
BF16 = jnp.bfloat16
F32 = jnp.float32


def call(body, outs, scratch, after=0, in_specs=None, out_specs=None):
    count = len(outs) if isinstance(outs, tuple) else 1

    def kernel(*refs):
        inputs = len(refs) - count - len(scratch)
        body(*refs[: inputs - after], *refs[inputs:])

    specs = {} if in_specs is None else {"in_specs": in_specs}
    specs |= {} if out_specs is None else {"out_specs": out_specs}
    return pl.pallas_call(
        kernel,
        out_shape=outs,
        scratch_shapes=scratch,
        compiler_params=pltpu.CompilerParams(vmem_limit_bytes=LIMIT),
        cost_estimate=pl.CostEstimate(flops=1 << 12, bytes_accessed=1 << 10, transcendentals=0),
        **specs,
    )


def width_shifts(rows):
    width = rows.shape[1]
    lane = lax.broadcasted_iota(jnp.int32, rows.shape, 1)
    none = jnp.zeros_like(rows)
    left = jnp.where(lane == 0, none, pltpu.roll(rows, 1, 1))
    right = jnp.where(lane == width - 1, none, pltpu.roll(rows, width - 1, 1))
    return (left, rows, right)


def row_turn(size, outer, inner):
    shift = inner.bit_length() - 1
    assert 1 << shift == inner and outer * inner == size
    row = lax.broadcasted_iota(jnp.int32, (size, size), 0)
    source = (row & (inner - 1)) * outer + (row >> shift)
    return jnp.where(lax.broadcasted_iota(jnp.int32, (size, size), 1) == source, 1.0, 0.0).astype(BF16)


def banded(first, width_tap, found, lane):
    channels, lanes = lane.shape
    for out_ref, block in found:
        rows = out_ref.shape[0] // TAPS
        rolled = {}
        for height in range(rows // channels):
            offset = channels * (height - 1)
            turn = offset % lanes
            if turn not in rolled:
                rolled[turn] = pltpu.roll(block, turn, 1) if turn else block
            for tile in range(rows // lanes):
                place = lane + (lanes * tile - offset)
                inside = (place >= 0) & (place < TAPS * channels)
                out_ref[
                    pl.ds(first + height * channels, channels),
                    width_tap * rows + tile * lanes : width_tap * rows + (tile + 1) * lanes,
                ] = jnp.where(inside, rolled[turn], 0.0).astype(BF16)


def strip(blocks):
    total = blocks[0]
    for place, block in enumerate(blocks[1:], 1):
        total = total + pltpu.roll(block, place * block.shape[0], 1)
    return total


def widened(source, wide):
    wide[...] = jnp.zeros_like(wide)
    for tap in range(source.shape[0]):
        wide[tap, :, : source.shape[2]] = source[tap].astype(F32)


def height_taps(depth_tap, width_tap):
    return [TAPS * TAPS * depth_tap + TAPS * height_tap + width_tap for height_tap in range(TAPS)]


def prepare_kernel(
    enc_hbm, dec_hbm, g0, g1, g2, g3, own_hbm, cot_hbm, dec_in_hbm, deep_hbm,
    enc_out, turn_out, back_out, columns_out, own_out, mine_out, dec_ref,
    enc_ref, row0, row1, row2, row3, sems, enc_wide,
):
    size = own_hbm.shape[0]
    channels = enc_ref.shape[1]
    rows_of = (row0, row1, row2, row3)
    copies = [
        pltpu.make_async_copy(source, target, sems.at[at])
        for at, (source, target) in enumerate(
            (
                (enc_hbm, enc_ref), (dec_hbm, dec_ref), *zip((g0, g1, g2, g3), rows_of, strict=True),
                (own_hbm, own_out), (cot_hbm, mine_out.at[:size]), (dec_in_hbm, mine_out.at[size : 2 * size]),
                (deep_hbm, mine_out.at[2 * size :]),
            )
        )
    ]
    for copy in copies:
        copy.start()
    lane = lax.broadcasted_iota(jnp.int32, (channels, enc_wide.shape[-1]), 1)
    turn_out[...] = row_turn(turn_out.shape[0], turn_out.shape[0] // channels, channels)
    back_out[...] = row_turn(back_out.shape[0], channels, back_out.shape[0] // channels)
    copies[0].wait()
    widened(enc_ref, enc_wide)

    @pl.loop(0, TAPS)
    def _(depth_tap):
        first = pl.multiple_of(depth_tap * (enc_out.shape[0] // TAPS), enc_out.shape[0] // TAPS)
        for width_tap in range(TAPS):
            taps = height_taps(depth_tap, width_tap)
            banded(first, width_tap, [(enc_out, strip([enc_wide[tap] for tap in taps]))], lane)

    for copy in copies[1:]:
        copy.wait()
    for place, row in enumerate(rows_of):
        columns_out[place] = jnp.broadcast_to(column(row), columns_out.shape[1:])


def weights_kernel(dec_ref, flip_out, up_out, down_out, wide):
    channels = dec_ref.shape[1]
    lanes = wide.shape[-1]
    lane = lax.broadcasted_iota(jnp.int32, (channels, lanes), 1)
    last = dec_ref.shape[0] - 1
    widened(dec_ref, wide)

    def first_half(block):
        return jnp.where(lane < channels, block, 0.0)

    def second_half(block):
        return first_half(pltpu.roll(block, lanes - channels, 1))

    def turned(blocks):
        stacked = jnp.concatenate(blocks + [jnp.zeros_like(blocks[0])] * (lanes // channels - TAPS), axis=0)
        return stacked.T[:channels]

    @pl.loop(0, TAPS)
    def _(depth_tap):
        first = pl.multiple_of(depth_tap * (flip_out.shape[0] // TAPS), flip_out.shape[0] // TAPS)
        for width_tap in range(TAPS):
            taps = height_taps(depth_tap, width_tap)
            found = [
                (up_out, strip([first_half(wide[tap]) for tap in taps])),
                (down_out, strip([second_half(wide[tap]) for tap in taps])),
                (flip_out, turned([second_half(wide[last - tap]) for tap in taps])),
            ]
            banded(first, width_tap, found, lane)


def column(row_ref):
    count = row_ref.shape[1]
    wide = jnp.broadcast_to(row_ref[...], (count, count))
    here = lax.broadcasted_iota(jnp.int32, (count, count), 0) == lax.broadcasted_iota(
        jnp.int32, (count, count), 1
    )
    return jnp.sum(jnp.where(here, wide, 0.0), axis=1, keepdims=True)


def turned_rows(pieces, turn_ref, turned_ref):
    side_by_side = jnp.concatenate([piece[...] for piece in pieces], axis=1)
    turned_ref[...] = jnp.dot(turn_ref[...], side_by_side, preferred_element_type=F32).astype(BF16)


def spread_depth(me, pieces, turn_ref, turned_ref, shifted_ref):
    rows = shifted_ref.shape[1] // TAPS
    width = shifted_ref.shape[2]
    depth = pieces[0].shape[0] // rows
    turned_rows(pieces, turn_ref, turned_ref)
    for distance in range(len(pieces)):
        owner = me ^ distance
        for layer in range(depth):
            cells = turned_ref[layer * rows : (layer + 1) * rows, distance * width : (distance + 1) * width]
            for tap, block in enumerate(width_shifts(cells)):
                shifted_ref[owner * depth + layer, tap * rows : (tap + 1) * rows, :] = block


def spread_height(me, pieces, turn_ref, turned_ref, shifted_ref):
    depth, rows, width = shifted_ref.shape
    rows = rows // TAPS
    part = pieces[0].shape[0] // depth
    turned_rows(pieces, turn_ref, turned_ref)
    for distance in range(len(pieces)):
        owner = me ^ distance
        for layer in range(depth):
            cells = turned_ref[layer * part : (layer + 1) * part, distance * width : (distance + 1) * width]
            for tap, block in enumerate(width_shifts(cells)):
                first = pl.multiple_of(tap * rows + owner * part, part)
                shifted_ref[layer, pl.ds(first, part), :] = block


def taps_product(pairs, parts_ref):
    depth = parts_ref.shape[0] - 2
    rows = parts_ref.shape[2]
    width = parts_ref.shape[3]
    for tap in range(TAPS):
        parts_ref[0, tap] = jnp.zeros((rows, width), F32)
        parts_ref[depth + 1, tap] = jnp.zeros((rows, width), F32)

    @pl.loop(0, depth // 2)
    def _(step):
        total = None
        for weights_ref, shifted_ref in pairs:
            cells = jnp.concatenate([shifted_ref[2 * step], shifted_ref[2 * step + 1]], axis=1)
            product = jnp.dot(weights_ref[...], cells, preferred_element_type=F32)
            total = product if total is None else total + product
        for tap in range(TAPS):
            block = total[tap * rows : (tap + 1) * rows]
            parts_ref[2 * step + 1, tap] = block[:, :width]
            parts_ref[2 * step + 2, tap] = block[:, width:]


def combined(parts_ref, layer):
    total = parts_ref[layer, 0]
    for tap in range(1, TAPS):
        total = total + parts_ref[layer + tap, tap]
    return total


def over_channels(sums, channels):
    total = sums[:channels]
    for first in range(channels, sums.shape[0], channels):
        total = total + sums[first : first + channels]
    return jnp.sum(total, axis=1, keepdims=True)


def tiled(values, count):
    return jnp.concatenate([values] * count, axis=0)


def normalized(parts_ref, pre_ref, sums_ref, channels):
    depth, rows, width = pre_ref.shape
    sums_ref[...] = jnp.zeros_like(sums_ref)

    @pl.loop(0, depth)
    def _(layer):
        pre = combined(parts_ref, layer)
        pre_ref[layer] = pre
        sums_ref[0] += pre
        sums_ref[1] += pre * pre

    cells = depth * (rows // channels) * width
    mean = over_channels(sums_ref[0], channels) * (1.0 / cells)
    square = over_channels(sums_ref[1], channels) * (1.0 / cells)
    return mean, lax.rsqrt(square - mean * mean + EPS)


def enc_kernel(
    channels, me_ref, p0, p1, p2, p3, weights_ref, turn_ref, columns_ref,
    shifted_ref, hat_ref, skip_ref, own_ref, scale_ref, turned_ref, parts_ref, pre_ref, sums_ref,
):
    me = me_ref[0]
    depth, rows, _ = pre_ref.shape
    spread_depth(me, (p0, p1, p2, p3), turn_ref, turned_ref, shifted_ref)
    taps_product([(weights_ref, shifted_ref)], parts_ref)
    mean, scale = normalized(parts_ref, pre_ref, sums_ref, channels)
    scale_ref[...] = jnp.broadcast_to(scale, scale_ref.shape)
    count = rows // channels
    means, scales = tiled(mean, count), tiled(scale, count)
    gains, biases = tiled(columns_ref[0, :, :1], count), tiled(columns_ref[1, :, :1], count)

    @pl.loop(0, depth)
    def _(layer):
        hat = (pre_ref[layer] - means) * scales
        hat_ref[layer] = hat
        skip_ref[layer] = jnp.maximum(gains * hat + biases, 0.0).astype(BF16)

    layers = own_ref.shape[0] // rows
    for layer in range(layers):
        own_ref[layer * rows : (layer + 1) * rows, :] = skip_ref[me * layers + layer]


def piece_views(refs, size, places):
    return [ref.at[place * size : (place + 1) * size] for ref, place in zip(refs, places, strict=True)]


def skip_grad_kernel(
    size, me_ref, p0, p1, p2, p3, weights_ref, turn_ref, grad_ref, cot_ref, shifted_ref, turned_ref, parts_ref
):
    rows = grad_ref.shape[1]
    spread_height(me_ref[0], piece_views((p0, p1, p2, p3), size, (0, 0, 0, 0)), turn_ref, turned_ref, shifted_ref)
    taps_product([(weights_ref, shifted_ref)], parts_ref)

    @pl.loop(0, grad_ref.shape[0])
    def _(layer):
        grad_ref[layer] = combined(parts_ref, layer).astype(BF16)
        cot_ref[layer] = shifted_ref[layer, rows : 2 * rows, :]


def dec_kernel(
    channels, size, me_ref, p0, p1, p2, p3, skip_ref, up_weights_ref, down_weights_ref, turn_ref,
    columns_ref, skip_own_ref, first_ref, second_ref, up_ref, down_ref, turned_ref, parts_ref, pre_ref, sums_ref,
):
    me = me_ref[0]
    depth, rows, _ = pre_ref.shape
    spread_height(me, piece_views((p0, p1, p2, p3), size, (1, 1, 1, 1)), turn_ref, turned_ref, up_ref)

    for layer in range(depth):
        for tap, block in enumerate(width_shifts(skip_ref[layer])):
            down_ref[layer, tap * rows : (tap + 1) * rows, :] = block

    taps_product([(up_weights_ref, up_ref), (down_weights_ref, down_ref)], parts_ref)
    mean, scale = normalized(parts_ref, pre_ref, sums_ref, channels)
    part = size // depth
    count = part // channels
    means, scales = tiled(mean, count), tiled(scale, count)
    gains, biases = tiled(columns_ref[2, :, :1], count), tiled(columns_ref[3, :, :1], count)

    own = []
    for layer in range(depth):
        pre = pre_ref[layer, pl.ds(pl.multiple_of(me * part, part), part), :]
        hat = (pre - means) * scales
        own.append(jnp.maximum(gains * hat + biases, 0.0).astype(BF16))
    own = jnp.concatenate(own, axis=0)
    even = (me_ref[2] & 1) == 0

    @pl.when(even)
    def _():
        first_ref[...] = skip_own_ref[...]
        second_ref[...] = own

    @pl.when(jnp.logical_not(even))
    def _():
        first_ref[...] = own
        second_ref[...] = skip_own_ref[...]


def outer_sums(channels, outers, padded_ref, shifted_refs, sums_ref):
    depth = shifted_refs[0].shape[0]
    rows = shifted_refs[0].shape[1] // TAPS
    lanes = len(shifted_refs) * TAPS * channels

    @pl.loop(0, rows // channels)
    def _(height):
        left = []
        for depth_tap, height_tap in outers:
            first = pl.multiple_of((height + 2 - height_tap) * channels, channels)
            left.append(
                jnp.concatenate(
                    [padded_ref[layer + 2 - depth_tap, pl.ds(first, channels), :] for layer in range(depth)],
                    axis=1,
                )
            )
        right = []
        for width_tap in range(TAPS):
            for shifted_ref in shifted_refs:
                first = pl.multiple_of(width_tap * rows + height * channels, channels)
                right.append(
                    jnp.concatenate(
                        [shifted_ref[layer, pl.ds(first, channels), :] for layer in range(depth)], axis=1
                    )
                )
        product = lax.dot_general(
            jnp.concatenate(left, axis=0),
            jnp.concatenate(right, axis=0),
            (((1,), (1,)), ((), ())),
            preferred_element_type=F32,
        )
        for tile in range(sums_ref.shape[0]):
            block = product[:, tile * 128 : min(lanes, (tile + 1) * 128)]
            old = sums_ref[tile, :, : block.shape[1]]
            sums_ref[tile, :, : block.shape[1]] = jnp.where(height == 0, 0.0, old) + block


def flattened(channels, sources, factor, sums_ref, flat_ref):
    lanes = flat_ref.shape[1]
    span = sources * channels
    merged = lanes // span
    count = channels // merged
    lane = lax.broadcasted_iota(jnp.int32, (count, lanes), 1)
    for outer in range(sums_ref.shape[1] // channels):
        for width_tap in range(TAPS):
            first = width_tap * span
            tile, inner = first // lanes, first % lanes
            total = None
            for row in range(merged):
                block = sums_ref[tile, pl.ds(outer * channels + row, count, stride=merged), :]
                turn = (row * span - inner) % lanes
                block = pltpu.roll(block, turn, 1) if turn else block
                total = block if total is None else jnp.where(lane >= row * span, block, total)
            start = (outer * TAPS + width_tap) * count
            flat_ref[start : start + count, :] = total * factor


def tap_sums(channels, factor, slabs, me_ref, padded_ref, shifted_refs, out_refs, sums_ref, flat_ref):
    blocks = TAPS * TAPS
    if len(out_refs) == 1:
        outers = [(outer // TAPS, outer % TAPS) for outer in range(blocks)]
    else:
        outers, offsets = [], []
        part = out_refs[0].shape[0]
        held = flat_ref.shape[0] // (PAIR * len(out_refs))
        for distance in range(len(out_refs)):
            place = ((me_ref[1] ^ distance) * slabs + me_ref[0]) * part
            first = place // held
            offsets.append(PAIR * distance * held + place - first * held)
            for outer in (first, jnp.minimum(first + 1, blocks - 1)):
                outers.append((outer // TAPS, outer % TAPS))
    outer_sums(channels, outers, padded_ref, shifted_refs, sums_ref)
    flattened(channels, len(shifted_refs), factor, sums_ref, flat_ref)
    if len(out_refs) == 1:
        out_refs[0][...] = flat_ref[...]
    else:
        for out_ref, offset in zip(out_refs, offsets, strict=True):
            out_ref[...] = flat_ref[pl.ds(offset, part), :].astype(out_ref.dtype)


def padded_rows(count):
    return -(-count // ROWS) * ROWS


def padded_cells(channels, cells_ref, padded_ref):
    depth, rows, _ = cells_ref.shape
    padded_ref[...] = jnp.zeros_like(padded_ref)

    @pl.loop(0, depth)
    def _(layer):
        padded_ref[layer + 1, channels : channels + rows, :] = cells_ref[layer]


def dec_grad_kernel(channels, factor, slabs, me_ref, cot_ref, up_ref, down_ref, *refs):
    *out_refs, padded_ref, sums_ref, flat_ref = refs
    padded_cells(channels, cot_ref, padded_ref)
    shifted_refs = (up_ref, down_ref)
    tap_sums(channels, factor, slabs, me_ref, padded_ref, shifted_refs, out_refs, sums_ref, flat_ref)


def enc_grad_kernel(
    channels, factor, slabs, me_ref, p0, p1, p2, p3, turn_ref, grad_ref, hat_ref, scale_ref, columns_ref,
    shifted_ref, *refs,
):
    *out_refs, turned_ref, gated_ref, acc_ref, padded_ref, sums_ref, flat_ref = refs
    dec_refs = []
    if len(out_refs) > 1:
        dec_refs, out_refs = out_refs[:PAIR], out_refs[PAIR:]
    me = me_ref[0]
    depth, rows, width = hat_ref.shape
    count = rows // channels
    gains, biases = tiled(columns_ref[0, :, :1], count), tiled(columns_ref[1, :, :1], count)
    acc_ref[...] = jnp.zeros_like(acc_ref)
    size = turn_ref.shape[0]
    layers = size // rows
    turned_rows(piece_views((p0, p1, p2, p3), size, (2, 2, 0, 0)), turn_ref, turned_ref)
    for distance in range(turned_ref.shape[1] // width):
        owner = me ^ distance
        piece = turned_ref.at[:, distance * width : (distance + 1) * width]
        for inner in range(layers):
            layer = owner * layers + inner
            hat = hat_ref[layer]
            upstream = grad_ref[layer].astype(F32) + piece[inner * rows : (inner + 1) * rows, :].astype(F32)
            gated = jnp.where(gains * hat + biases > 0, upstream, 0.0) * gains
            gated_ref[layer] = gated
            acc_ref[0] += gated
            acc_ref[1] += gated * hat
    cells = depth * count * width
    first = tiled(over_channels(acc_ref[0], channels) * (1.0 / cells), count)
    second = tiled(over_channels(acc_ref[1], channels) * (1.0 / cells), count)
    scales = tiled(scale_ref[:, :1], count)
    padded_ref[...] = jnp.zeros_like(padded_ref)

    @pl.loop(0, depth)
    def _(layer):
        grad = (gated_ref[layer] - first - hat_ref[layer] * second) * scales
        padded_ref[layer + 1, channels : channels + rows, :] = grad.astype(BF16)

    own_refs = list(out_refs)
    for at, dec_ref in enumerate(dec_refs):
        count = dec_ref.shape[0]
        start = padded_rows(count)
        out_refs[at][...] = jnp.zeros(out_refs[at].shape, out_refs[at].dtype)
        out_refs[at][:count, :] = dec_ref[...].astype(out_refs[at].dtype)
        own_refs[at] = out_refs[at].at[start : start + count // PAIR]
    tap_sums(channels, factor, slabs, me_ref, padded_ref, (shifted_ref,), own_refs, sums_ref, flat_ref)


def swapped(block, distance):
    count = lax.axis_size("space")
    return lax.ppermute(block, "space", [(i, i ^ distance) for i in range(count)])


def paired(block, start):
    count, copies = lax.axis_size("section"), lax.axis_size("dp")
    route = []
    for section in range(count):
        upper = (section - start) % 2
        partner = section - 1 if upper else section + 1
        for copy in range(copies):
            to = (partner, copy) if start <= min(section, partner) and partner < count else (section, copy ^ 1)
            if to[1] < copies:
                route.append((section * copies + copy, to[0] * copies + to[1]))
    return lax.ppermute(block, ("section", "dp"), route)


def halves(rows):
    count = lax.axis_size("dp") * lax.axis_size("space")
    blocks = TAPS * TAPS
    part, held = rows // count, rows // blocks
    return (
        lax.axis_size("dp") == PAIR
        and rows % count == 0
        and all((place + 1) * part <= (place * part // held + PAIR) * held for place in range(count))
    )


def scattered(flat):
    count, slabs = lax.axis_size("dp"), lax.axis_size("space")
    every = flat.reshape(count, slabs, -1)
    mine = lax.dynamic_index_in_dim(every, lax.axis_index("space"), 1, keepdims=False)
    return lax.psum_scatter(mine, "dp", scatter_dimension=0, tiled=True)


def put_kernel(sections, me_ref, back_ref, first_ref, second_ref, enc_out, dec_out):
    width = enc_out.shape[1]
    section = me_ref[2]
    even = (section & 1) == 0
    both = jnp.concatenate([first_ref[...], second_ref[...]], axis=1)
    both = jnp.dot(back_ref[...], both, preferred_element_type=F32)
    first, second = both[:, :width], both[:, width:]
    enc = jnp.where(even, second, first)
    dec = jnp.where(even, first, second)
    enc_out[...] = jnp.where(section == 0, 0.0, enc).astype(BF16)
    dec_out[...] = jnp.where(section == sections - 1, 0.0, dec).astype(BF16)


def finish_kernel(kept_ref, received_ref, *outs):
    first = 0
    for out in outs:
        lanes = kept_ref.shape[1]
        count = out.shape[1] // lanes
        end = first + padded_rows(count)
        total = kept_ref[first:end, :] + received_ref[first:end, :].astype(F32)
        for row in range(count):
            out[:, row * lanes : (row + 1) * lanes] = total[row : row + 1]
        first = end


def body(
    enc_input, dec_input, dec_cotangent, deep_cotangent, enc_weight, dec_weight,
    enc_gain, enc_bias, dec_gain, dec_bias,
):
    _, _, channels, slab_depth, height, width = enc_input.shape
    slabs = lax.axis_size("space")
    depth = slab_depth * slabs
    slab_height = height // slabs
    rows = channels * height
    voxels = depth * height * width
    factor = 1.0 / math.sqrt(lax.axis_size("dp") * voxels)
    me = jnp.stack([lax.axis_index("space"), lax.axis_index("dp"), lax.axis_index("section")]).astype(jnp.int32)

    shape = pltpu.VMEM
    size = channels * slab_depth * height
    far, near = slabs // 2, slabs // 4
    enc_raw, cot_raw, dec_raw, deep_raw = (
        cells.reshape(size, width) for cells in (enc_input, dec_cotangent, dec_input, deep_cotangent)
    )
    enc_far = swapped(enc_raw, far)
    enc_near = swapped(enc_raw, near)

    square = shape((size, size), BF16)
    matrix = shape((TAPS * rows, TAPS * rows), BF16)
    small = pltpu.VMEM((1, channels), F32)
    wide = pltpu.VMEM((enc_weight.shape[1], channels, 128), F32)
    enc_banded, turn, back, columns, enc_own, mine, dec_taps = call(
        prepare_kernel,
        (
            matrix, square, square, shape((4, channels, 128), F32), shape((size, width), BF16),
            shape((3 * size, width), BF16), shape(dec_weight.shape[1:], BF16),
        ),
        [
            pltpu.VMEM(enc_weight.shape[1:], BF16), small, small, small, small,
            pltpu.SemaphoreType.DMA((10,)), wide,
        ],
        1,
        [pl.BlockSpec(memory_space=pltpu.HBM)] * 10 + [pl.BlockSpec(memory_space=pltpu.SMEM)],
    )(
        *(
            pltpu.with_memory_space_constraint(array, pltpu.HBM)
            for array in (
                enc_weight[0], dec_weight[0], enc_gain, enc_bias, dec_gain, dec_bias,
                enc_raw, cot_raw, dec_raw, deep_raw,
            )
        ),
        me,
    )
    pair_far = swapped(mine[: 2 * size], far)
    others_near = swapped(mine, near)
    enc_relay = swapped(enc_far, near)
    flip_banded, up_banded, down_banded = call(weights_kernel, (matrix, matrix, matrix), [wide])(dec_taps)
    pair_relay = swapped(pair_far, near)

    shifted_shape = (depth, TAPS * rows, width)
    cell_shape = (depth, rows, width)
    turned = pltpu.VMEM((size, slabs * width), BF16)
    parts = pltpu.VMEM((depth + 2, TAPS, rows, width), F32)
    padded = pltpu.VMEM((depth + 2, rows + 2 * channels, width), BF16)
    pre, line_sums = pltpu.VMEM(cell_shape, F32), pltpu.VMEM((2, rows, width), F32)
    enc_shifted, hat, skip, skip_own, scale = call(
        functools.partial(enc_kernel, channels),
        (
            shape(shifted_shape, BF16),
            shape(cell_shape, F32),
            shape(cell_shape, BF16),
            shape((size, width), BF16),
            shape((channels, 128), F32),
        ),
        [turned, parts, pre, line_sums],
    )(me, enc_own, enc_near, enc_far, enc_relay, enc_banded, turn, columns)
    deep_far = swapped(lax.optimization_barrier((deep_raw, scale))[0], far)
    deep_relay = swapped(deep_far, near)
    skip_grad, cot = call(
        functools.partial(skip_grad_kernel, size),
        (shape(cell_shape, BF16), shape(cell_shape, BF16)),
        [pltpu.VMEM(shifted_shape, BF16), turned, parts],
        1,
    )(me, mine, others_near, pair_far, pair_relay, flip_banded, turn, scale)

    first, second, up, down = call(
        functools.partial(dec_kernel, channels, size),
        (shape((size, width), BF16),) * 2 + (shape(shifted_shape, BF16),) * 2,
        [turned, parts, pre, line_sums],
        1,
    )(
        me, mine, others_near, pair_far, pair_relay, skip, up_banded, down_banded, turn, columns,
        skip_own, skip_grad,
    )
    first = paired(first, 0)

    flat_rows = TAPS * TAPS * TAPS * channels * channels // 128
    pair = halves(flat_rows) and halves(2 * flat_rows)

    dec_rows, enc_rows = 2 * flat_rows // (PAIR * slabs), flat_rows // (PAIR * slabs)
    both_rows = padded_rows(dec_rows) + padded_rows(enc_rows)

    def grad_shapes(total):
        if not pair:
            return (shape((total, 128), F32),)
        return (shape((total // (PAIR * slabs), 128), F32),) * 2

    def grad_scratch(total, tiles):
        outers = 2 * PAIR if pair else TAPS * TAPS
        held = total // (TAPS * TAPS) * outers
        return [padded, pltpu.VMEM((tiles, outers * channels, 128), F32), pltpu.VMEM((held, 128), F32)]

    dec_flat = call(
        functools.partial(dec_grad_kernel, channels, factor, slabs),
        grad_shapes(2 * flat_rows),
        grad_scratch(2 * flat_rows, 2),
    )(me, cot, up, down)
    second = paired(lax.optimization_barrier((second, dec_flat[0]))[0], 1)
    enc_flat = call(
        functools.partial(enc_grad_kernel, channels, factor, slabs),
        (shape((both_rows, 128), F32), shape((both_rows, 128), BF16))
        if pair
        else grad_shapes(flat_rows),
        [turned, pre, line_sums, *grad_scratch(flat_rows, 1)],
        0 if pair else 1,
    )(
        me, mine, others_near, deep_far, deep_relay, turn, skip_grad, hat, scale, columns, enc_shifted,
        *dec_flat,
    )

    moved = jax.ShapeDtypeStruct((size, width), BF16)
    enc_handoff, dec_handoff = call(
        functools.partial(put_kernel, lax.axis_size("section")), (moved, moved), [], 1
    )(me, back, first, second, enc_flat[0])
    if pair:
        kept, sent = enc_flat
        received = lax.ppermute(sent, "dp", [(0, 1), (1, 0)])
        ends = tuple(jax.ShapeDtypeStruct((1, count * 128), F32) for count in (dec_rows, enc_rows))
        grads = call(finish_kernel, ends, [])(kept, received)
    else:
        grads = [scattered(dec_flat[0]), scattered(enc_flat[0])]
    enc_handoff = enc_handoff.reshape(1, 1, channels, slab_depth, height, width)
    dec_handoff = dec_handoff.reshape(1, 1, channels, depth, slab_height, width)
    return (enc_handoff, dec_handoff, grads[1].reshape(1, -1), grads[0].reshape(1, -1))


def solution(mesh):
    in_specs = (
        P("section", "dp", None, "space", None, None),
        P("section", "dp", None, None, "space", None),
        P("section", "dp", None, None, "space", None),
        P("section", "dp", None, "space", None, None),
        P("section", None, None, None),
        P("section", None, None, None),
        P("section", None),
        P("section", None),
        P("section", None),
        P("section", None),
    )
    out_specs = (
        P("section", "dp", None, "space", None, None),
        P("section", "dp", None, None, "space", None),
        P("section", ("dp", "space")),
        P("section", ("dp", "space")),
    )

    return jax.shard_map(body, mesh=mesh, in_specs=in_specs, out_specs=out_specs, check_vma=False)
```

```python
import functools
import math

import jax
import jax.numpy as jnp
from jax import lax
from jax.experimental import pallas as pl
from jax.experimental.pallas import tpu as pltpu
from jax.sharding import PartitionSpec as P


EPS = 1e-05
TAPS = 3
PAIR = 2
ROWS = 16
GROUP = 8
HEIGHTS = 4
LIMIT = 12 * 1024 * 1024
BF16 = jnp.bfloat16
F32 = jnp.float32


def call(body, outs, scratch, after=0, in_specs=None, out_specs=None):
    count = len(outs) if isinstance(outs, tuple) else 1

    def kernel(*refs):
        inputs = len(refs) - count - len(scratch)
        body(*refs[: inputs - after], *refs[inputs:])

    specs = {} if in_specs is None else {"in_specs": in_specs}
    specs |= {} if out_specs is None else {"out_specs": out_specs}
    return pl.pallas_call(
        kernel,
        out_shape=outs,
        scratch_shapes=scratch,
        compiler_params=pltpu.CompilerParams(vmem_limit_bytes=LIMIT),
        cost_estimate=pl.CostEstimate(flops=1 << 12, bytes_accessed=1 << 10, transcendentals=0),
        **specs,
    )


def width_shifts(rows):
    width = rows.shape[1]
    lane = lax.broadcasted_iota(jnp.int32, rows.shape, 1)
    none = jnp.zeros_like(rows)
    left = jnp.where(lane == 0, none, pltpu.roll(rows, 1, 1))
    right = jnp.where(lane == width - 1, none, pltpu.roll(rows, width - 1, 1))
    return (left, rows, right)


def row_turn(size, outer, inner):
    shift = inner.bit_length() - 1
    assert 1 << shift == inner and outer * inner == size
    row = lax.broadcasted_iota(jnp.int32, (size, size), 0)
    source = (row & (inner - 1)) * outer + (row >> shift)
    return jnp.where(lax.broadcasted_iota(jnp.int32, (size, size), 1) == source, 1.0, 0.0).astype(BF16)


def banded(first, width_tap, found, lane):
    channels, lanes = lane.shape
    for out_ref, block in found:
        rows = out_ref.shape[0] // TAPS
        rolled = {}
        for height in range(rows // channels):
            offset = channels * (height - 1)
            turn = offset % lanes
            if turn not in rolled:
                rolled[turn] = pltpu.roll(block, turn, 1) if turn else block
            for tile in range(rows // lanes):
                place = lane + (lanes * tile - offset)
                inside = (place >= 0) & (place < TAPS * channels)
                out_ref[
                    pl.ds(first + height * channels, channels),
                    width_tap * rows + tile * lanes : width_tap * rows + (tile + 1) * lanes,
                ] = jnp.where(inside, rolled[turn], 0.0).astype(BF16)


def strip(blocks):
    total = blocks[0]
    for place, block in enumerate(blocks[1:], 1):
        total = total + pltpu.roll(block, place * block.shape[0], 1)
    return total


def widened(source, wide):
    wide[...] = jnp.zeros_like(wide)
    for tap in range(source.shape[0]):
        wide[tap, :, : source.shape[2]] = source[tap].astype(F32)


def height_taps(depth_tap, width_tap):
    return [TAPS * TAPS * depth_tap + TAPS * height_tap + width_tap for height_tap in range(TAPS)]


def prepare_kernel(
    enc_hbm, dec_hbm, g0, g1, g2, g3, own_hbm, cot_hbm, dec_in_hbm, deep_hbm,
    enc_out, turn_out, back_out, columns_out, own_out, mine_out, dec_ref,
    enc_ref, row0, row1, row2, row3, sems, enc_wide,
):
    size = own_hbm.shape[0]
    channels = enc_ref.shape[1]
    rows_of = (row0, row1, row2, row3)
    copies = [
        pltpu.make_async_copy(source, target, sems.at[at])
        for at, (source, target) in enumerate(
            (
                (enc_hbm, enc_ref), (dec_hbm, dec_ref), *zip((g0, g1, g2, g3), rows_of, strict=True),
                (own_hbm, own_out), (cot_hbm, mine_out.at[:size]), (dec_in_hbm, mine_out.at[size : 2 * size]),
                (deep_hbm, mine_out.at[2 * size :]),
            )
        )
    ]
    for copy in copies:
        copy.start()
    lane = lax.broadcasted_iota(jnp.int32, (channels, enc_wide.shape[-1]), 1)
    turn_out[...] = row_turn(turn_out.shape[0], turn_out.shape[0] // channels, channels)
    back_out[...] = row_turn(back_out.shape[0], channels, back_out.shape[0] // channels)
    copies[0].wait()
    widened(enc_ref, enc_wide)

    @pl.loop(0, TAPS)
    def _(depth_tap):
        first = pl.multiple_of(depth_tap * (enc_out.shape[0] // TAPS), enc_out.shape[0] // TAPS)
        for width_tap in range(TAPS):
            taps = height_taps(depth_tap, width_tap)
            banded(first, width_tap, [(enc_out, strip([enc_wide[tap] for tap in taps]))], lane)

    for copy in copies[1:]:
        copy.wait()
    for place, row in enumerate(rows_of):
        columns_out[place] = jnp.broadcast_to(column(row), columns_out.shape[1:])


def weights_kernel(dec_ref, flip_out, up_out, down_out, wide):
    channels = dec_ref.shape[1]
    lanes = wide.shape[-1]
    lane = lax.broadcasted_iota(jnp.int32, (channels, lanes), 1)
    last = dec_ref.shape[0] - 1
    widened(dec_ref, wide)

    def first_half(block):
        return jnp.where(lane < channels, block, 0.0)

    def second_half(block):
        return first_half(pltpu.roll(block, lanes - channels, 1))

    def turned(blocks):
        stacked = jnp.concatenate(blocks + [jnp.zeros_like(blocks[0])] * (lanes // channels - TAPS), axis=0)
        return stacked.T[:channels]

    @pl.loop(0, TAPS)
    def _(depth_tap):
        first = pl.multiple_of(depth_tap * (flip_out.shape[0] // TAPS), flip_out.shape[0] // TAPS)
        for width_tap in range(TAPS):
            taps = height_taps(depth_tap, width_tap)
            found = [
                (up_out, strip([first_half(wide[tap]) for tap in taps])),
                (down_out, strip([second_half(wide[tap]) for tap in taps])),
                (flip_out, turned([second_half(wide[last - tap]) for tap in taps])),
            ]
            banded(first, width_tap, found, lane)


def column(row_ref):
    count = row_ref.shape[1]
    wide = jnp.broadcast_to(row_ref[...], (count, count))
    here = lax.broadcasted_iota(jnp.int32, (count, count), 0) == lax.broadcasted_iota(
        jnp.int32, (count, count), 1
    )
    return jnp.sum(jnp.where(here, wide, 0.0), axis=1, keepdims=True)


def turned_rows(pieces, turn_ref, turned_ref):
    side_by_side = jnp.concatenate([piece[...] for piece in pieces], axis=1)
    turned_ref[...] = jnp.dot(turn_ref[...], side_by_side, preferred_element_type=F32).astype(BF16)


def spread_depth(me, pieces, turn_ref, turned_ref, shifted_ref):
    rows = shifted_ref.shape[1] // TAPS
    width = shifted_ref.shape[2]
    depth = pieces[0].shape[0] // rows
    turned_rows(pieces, turn_ref, turned_ref)
    for distance in range(len(pieces)):
        owner = me ^ distance
        for layer in range(depth):
            cells = turned_ref[layer * rows : (layer + 1) * rows, distance * width : (distance + 1) * width]
            for tap, block in enumerate(width_shifts(cells)):
                shifted_ref[owner * depth + layer, tap * rows : (tap + 1) * rows, :] = block


def spread_height(me, pieces, turn_ref, turned_ref, shifted_ref):
    depth, rows, width = shifted_ref.shape
    rows = rows // TAPS
    part = pieces[0].shape[0] // depth
    turned_rows(pieces, turn_ref, turned_ref)
    for distance in range(len(pieces)):
        owner = me ^ distance
        for layer in range(depth):
            cells = turned_ref[layer * part : (layer + 1) * part, distance * width : (distance + 1) * width]
            for tap, block in enumerate(width_shifts(cells)):
                first = pl.multiple_of(tap * rows + owner * part, part)
                shifted_ref[layer, pl.ds(first, part), :] = block


def taps_product(pairs, parts_ref):
    depth = parts_ref.shape[0] - 2
    rows = parts_ref.shape[2]
    width = parts_ref.shape[3]
    for tap in range(TAPS):
        parts_ref[0, tap] = jnp.zeros((rows, width), F32)
        parts_ref[depth + 1, tap] = jnp.zeros((rows, width), F32)

    group = GROUP if depth % GROUP == 0 else 1

    @pl.loop(0, depth // group)
    def _(step):
        total = None
        for weights_ref, shifted_ref in pairs:
            cells = jnp.concatenate([shifted_ref[group * step + inner] for inner in range(group)], axis=1)
            product = jnp.dot(weights_ref[...], cells, preferred_element_type=F32)
            total = product if total is None else total + product
        for tap in range(TAPS):
            block = total[tap * rows : (tap + 1) * rows]
            for inner in range(group):
                parts_ref[group * step + 1 + inner, tap] = block[:, inner * width : (inner + 1) * width]


def combined(parts_ref, layer):
    total = parts_ref[layer, 0]
    for tap in range(1, TAPS):
        total = total + parts_ref[layer + tap, tap]
    return total


def over_channels(sums, channels):
    total = sums[:channels]
    for first in range(channels, sums.shape[0], channels):
        total = total + sums[first : first + channels]
    return jnp.sum(total, axis=1, keepdims=True)


def tiled(values, count):
    return jnp.concatenate([values] * count, axis=0)


def normalized(parts_ref, pre_ref, sums_ref, channels):
    depth, rows, width = pre_ref.shape
    sums_ref[...] = jnp.zeros_like(sums_ref)

    @pl.loop(0, rows // channels)
    def _(height):
        part = pl.ds(pl.multiple_of(height * channels, channels), channels)
        total, squares = jnp.zeros((channels, width), F32), jnp.zeros((channels, width), F32)
        for layer in range(depth):
            pre = parts_ref[layer, 0, part, :]
            for tap in range(1, TAPS):
                pre = pre + parts_ref[layer + tap, tap, part, :]
            pre_ref[layer, part, :] = pre
            total = total + pre
            squares = squares + pre * pre
        sums_ref[0] += total
        sums_ref[1] += squares

    cells = depth * (rows // channels) * width
    mean = jnp.sum(sums_ref[0], axis=1, keepdims=True) * (1.0 / cells)
    square = jnp.sum(sums_ref[1], axis=1, keepdims=True) * (1.0 / cells)
    return mean, lax.rsqrt(square - mean * mean + EPS)


def enc_kernel(
    channels, me_ref, p0, p1, p2, p3, weights_ref, turn_ref, columns_ref,
    shifted_ref, hat_ref, skip_ref, own_ref, scale_ref, turned_ref, parts_ref, pre_ref, sums_ref,
):
    me = me_ref[0]
    depth, rows, _ = pre_ref.shape
    spread_depth(me, (p0, p1, p2, p3), turn_ref, turned_ref, shifted_ref)
    taps_product([(weights_ref, shifted_ref)], parts_ref)
    mean, scale = normalized(parts_ref, pre_ref, sums_ref, channels)
    scale_ref[...] = jnp.broadcast_to(scale, scale_ref.shape)
    count = rows // channels
    means, scales = tiled(mean, count), tiled(scale, count)
    gains, biases = tiled(columns_ref[0, :, :1], count), tiled(columns_ref[1, :, :1], count)

    for layer in range(depth):
        hat = (pre_ref[layer] - means) * scales
        hat_ref[layer] = hat
        skip_ref[layer] = jnp.maximum(gains * hat + biases, 0.0).astype(BF16)

    layers = own_ref.shape[0] // rows
    for layer in range(layers):
        own_ref[layer * rows : (layer + 1) * rows, :] = skip_ref[me * layers + layer]


def piece_views(refs, size, places):
    return [ref.at[place * size : (place + 1) * size] for ref, place in zip(refs, places, strict=True)]


def skip_grad_kernel(
    size, me_ref, p0, p1, p2, p3, weights_ref, turn_ref, grad_ref, cot_ref, shifted_ref, turned_ref, parts_ref
):
    rows = grad_ref.shape[1]
    spread_height(me_ref[0], piece_views((p0, p1, p2, p3), size, (0, 0, 0, 0)), turn_ref, turned_ref, shifted_ref)
    taps_product([(weights_ref, shifted_ref)], parts_ref)

    @pl.loop(0, grad_ref.shape[0])
    def _(layer):
        grad_ref[layer] = combined(parts_ref, layer).astype(BF16)
        cot_ref[layer] = shifted_ref[layer, rows : 2 * rows, :]


def dec_kernel(
    channels, size, me_ref, p0, p1, p2, p3, skip_ref, up_weights_ref, down_weights_ref, turn_ref,
    columns_ref, skip_own_ref, first_ref, second_ref, up_ref, down_ref, turned_ref, parts_ref, pre_ref, sums_ref,
):
    me = me_ref[0]
    depth, rows, _ = pre_ref.shape
    spread_height(me, piece_views((p0, p1, p2, p3), size, (1, 1, 1, 1)), turn_ref, turned_ref, up_ref)

    for layer in range(depth):
        for tap, block in enumerate(width_shifts(skip_ref[layer])):
            down_ref[layer, tap * rows : (tap + 1) * rows, :] = block

    taps_product([(up_weights_ref, up_ref), (down_weights_ref, down_ref)], parts_ref)
    mean, scale = normalized(parts_ref, pre_ref, sums_ref, channels)
    part = size // depth
    count = part // channels
    means, scales = tiled(mean, count), tiled(scale, count)
    gains, biases = tiled(columns_ref[2, :, :1], count), tiled(columns_ref[3, :, :1], count)

    own = []
    for layer in range(depth):
        pre = pre_ref[layer, pl.ds(pl.multiple_of(me * part, part), part), :]
        hat = (pre - means) * scales
        own.append(jnp.maximum(gains * hat + biases, 0.0).astype(BF16))
    own = jnp.concatenate(own, axis=0)
    even = (me_ref[2] & 1) == 0

    @pl.when(even)
    def _():
        first_ref[...] = skip_own_ref[...]
        second_ref[...] = own

    @pl.when(jnp.logical_not(even))
    def _():
        first_ref[...] = own
        second_ref[...] = skip_own_ref[...]


def outer_sums(channels, outers, padded_ref, shifted_refs, sums_ref):
    depth = shifted_refs[0].shape[0]
    rows = shifted_refs[0].shape[1] // TAPS
    lanes = len(shifted_refs) * TAPS * channels

    every = rows // channels
    group = HEIGHTS * len(shifted_refs)
    group = group if every % group == 0 else 1

    @pl.loop(0, every // group)
    def _(step):
        heights = [group * step + inner for inner in range(group)]
        left = []
        for depth_tap, height_tap in outers:
            cells = []
            for height in heights:
                first = pl.multiple_of((height + 2 - height_tap) * channels, channels)
                cells += [padded_ref[layer + 2 - depth_tap, pl.ds(first, channels), :] for layer in range(depth)]
            left.append(jnp.concatenate(cells, axis=1))
        right = []
        for width_tap in range(TAPS):
            for shifted_ref in shifted_refs:
                cells = []
                for height in heights:
                    first = pl.multiple_of(width_tap * rows + height * channels, channels)
                    cells += [shifted_ref[layer, pl.ds(first, channels), :] for layer in range(depth)]
                right.append(jnp.concatenate(cells, axis=1))
        product = lax.dot_general(
            jnp.concatenate(left, axis=0),
            jnp.concatenate(right, axis=0),
            (((1,), (1,)), ((), ())),
            preferred_element_type=F32,
        )
        for tile in range(sums_ref.shape[0]):
            block = product[:, tile * 128 : min(lanes, (tile + 1) * 128)]
            old = sums_ref[tile, :, : block.shape[1]]
            sums_ref[tile, :, : block.shape[1]] = jnp.where(step == 0, 0.0, old) + block


def flattened(channels, sources, factor, sums_ref, flat_ref):
    lanes = flat_ref.shape[1]
    span = sources * channels
    merged = lanes // span
    count = channels // merged
    lane = lax.broadcasted_iota(jnp.int32, (count, lanes), 1)
    for outer in range(sums_ref.shape[1] // channels):
        for width_tap in range(TAPS):
            first = width_tap * span
            tile, inner = first // lanes, first % lanes
            total = None
            for row in range(merged):
                block = sums_ref[tile, pl.ds(outer * channels + row, count, stride=merged), :]
                turn = (row * span - inner) % lanes
                block = pltpu.roll(block, turn, 1) if turn else block
                total = block if total is None else jnp.where(lane >= row * span, block, total)
            start = (outer * TAPS + width_tap) * count
            flat_ref[start : start + count, :] = total * factor


def tap_sums(channels, factor, slabs, me_ref, padded_ref, shifted_refs, out_refs, sums_ref, flat_ref):
    blocks = TAPS * TAPS
    if len(out_refs) == 1:
        outers = [(outer // TAPS, outer % TAPS) for outer in range(blocks)]
    else:
        outers, offsets = [], []
        part = out_refs[0].shape[0]
        held = flat_ref.shape[0] // (PAIR * len(out_refs))
        for distance in range(len(out_refs)):
            place = ((me_ref[1] ^ distance) * slabs + me_ref[0]) * part
            first = place // held
            offsets.append(PAIR * distance * held + place - first * held)
            for outer in (first, jnp.minimum(first + 1, blocks - 1)):
                outers.append((outer // TAPS, outer % TAPS))
    outer_sums(channels, outers, padded_ref, shifted_refs, sums_ref)
    flattened(channels, len(shifted_refs), factor, sums_ref, flat_ref)
    if len(out_refs) == 1:
        out_refs[0][...] = flat_ref[...]
    else:
        for out_ref, offset in zip(out_refs, offsets, strict=True):
            out_ref[...] = flat_ref[pl.ds(offset, part), :].astype(out_ref.dtype)


def padded_rows(count):
    return -(-count // ROWS) * ROWS


def padded_cells(channels, cells_ref, padded_ref):
    depth, rows, _ = cells_ref.shape
    padded_ref[...] = jnp.zeros_like(padded_ref)

    @pl.loop(0, depth)
    def _(layer):
        padded_ref[layer + 1, channels : channels + rows, :] = cells_ref[layer]


def dec_grad_kernel(channels, factor, slabs, me_ref, cot_ref, up_ref, down_ref, *refs):
    *out_refs, padded_ref, sums_ref, flat_ref = refs
    padded_cells(channels, cot_ref, padded_ref)
    shifted_refs = (up_ref, down_ref)
    tap_sums(channels, factor, slabs, me_ref, padded_ref, shifted_refs, out_refs, sums_ref, flat_ref)


def enc_grad_kernel(
    channels, factor, slabs, me_ref, p0, p1, p2, p3, turn_ref, grad_ref, hat_ref, scale_ref, columns_ref,
    shifted_ref, *refs,
):
    *out_refs, turned_ref, gated_ref, acc_ref, padded_ref, sums_ref, flat_ref = refs
    dec_refs = []
    if len(out_refs) > 1:
        dec_refs, out_refs = out_refs[:PAIR], out_refs[PAIR:]
    me = me_ref[0]
    depth, rows, width = hat_ref.shape
    count = rows // channels
    gains, biases = tiled(columns_ref[0, :, :1], count), tiled(columns_ref[1, :, :1], count)
    acc_ref[...] = jnp.zeros_like(acc_ref)
    size = turn_ref.shape[0]
    layers = size // rows
    turned_rows(piece_views((p0, p1, p2, p3), size, (2, 2, 0, 0)), turn_ref, turned_ref)
    for distance in range(turned_ref.shape[1] // width):
        owner = me ^ distance
        piece = turned_ref.at[:, distance * width : (distance + 1) * width]
        for inner in range(layers):
            layer = owner * layers + inner
            hat = hat_ref[layer]
            upstream = grad_ref[layer].astype(F32) + piece[inner * rows : (inner + 1) * rows, :].astype(F32)
            gated = jnp.where(gains * hat + biases > 0, upstream, 0.0) * gains
            gated_ref[layer] = gated
            acc_ref[0] += gated
            acc_ref[1] += gated * hat
    cells = depth * count * width
    first = tiled(over_channels(acc_ref[0], channels) * (1.0 / cells), count)
    second = tiled(over_channels(acc_ref[1], channels) * (1.0 / cells), count)
    scales = tiled(scale_ref[:, :1], count)
    padded_ref[...] = jnp.zeros_like(padded_ref)

    @pl.loop(0, depth)
    def _(layer):
        grad = (gated_ref[layer] - first - hat_ref[layer] * second) * scales
        padded_ref[layer + 1, channels : channels + rows, :] = grad.astype(BF16)

    own_refs = list(out_refs)
    for at, dec_ref in enumerate(dec_refs):
        count = dec_ref.shape[0]
        start = padded_rows(count)
        out_refs[at][...] = jnp.zeros(out_refs[at].shape, out_refs[at].dtype)
        out_refs[at][:count, :] = dec_ref[...].astype(out_refs[at].dtype)
        own_refs[at] = out_refs[at].at[start : start + count // PAIR]
    tap_sums(channels, factor, slabs, me_ref, padded_ref, (shifted_ref,), own_refs, sums_ref, flat_ref)


def swapped(block, distance):
    count = lax.axis_size("space")
    return lax.ppermute(block, "space", [(i, i ^ distance) for i in range(count)])


def paired(block, start):
    count, copies = lax.axis_size("section"), lax.axis_size("dp")
    route = []
    for section in range(count):
        upper = (section - start) % 2
        partner = section - 1 if upper else section + 1
        for copy in range(copies):
            to = (partner, copy) if start <= min(section, partner) and partner < count else (section, copy ^ 1)
            if to[1] < copies:
                route.append((section * copies + copy, to[0] * copies + to[1]))
    return lax.ppermute(block, ("section", "dp"), route)


def halves(rows):
    count = lax.axis_size("dp") * lax.axis_size("space")
    blocks = TAPS * TAPS
    part, held = rows // count, rows // blocks
    return (
        lax.axis_size("dp") == PAIR
        and rows % count == 0
        and all((place + 1) * part <= (place * part // held + PAIR) * held for place in range(count))
    )


def scattered(flat):
    count, slabs = lax.axis_size("dp"), lax.axis_size("space")
    every = flat.reshape(count, slabs, -1)
    mine = lax.dynamic_index_in_dim(every, lax.axis_index("space"), 1, keepdims=False)
    return lax.psum_scatter(mine, "dp", scatter_dimension=0, tiled=True)


def put_kernel(sections, me_ref, back_ref, first_ref, second_ref, enc_out, dec_out):
    width = enc_out.shape[1]
    section = me_ref[2]
    even = (section & 1) == 0
    both = jnp.concatenate([first_ref[...], second_ref[...]], axis=1)
    both = jnp.dot(back_ref[...], both, preferred_element_type=F32)
    first, second = both[:, :width], both[:, width:]
    enc = jnp.where(even, second, first)
    dec = jnp.where(even, first, second)
    enc_out[...] = jnp.where(section == 0, 0.0, enc).astype(BF16)
    dec_out[...] = jnp.where(section == sections - 1, 0.0, dec).astype(BF16)


def finish_kernel(kept_ref, received_ref, *outs):
    first = 0
    for out in outs:
        lanes = kept_ref.shape[1]
        count = out.shape[1] // lanes
        end = first + padded_rows(count)
        total = kept_ref[first:end, :] + received_ref[first:end, :].astype(F32)
        for row in range(count):
            out[:, row * lanes : (row + 1) * lanes] = total[row : row + 1]
        first = end


def body(
    enc_input, dec_input, dec_cotangent, deep_cotangent, enc_weight, dec_weight,
    enc_gain, enc_bias, dec_gain, dec_bias,
):
    _, _, channels, slab_depth, height, width = enc_input.shape
    slabs = lax.axis_size("space")
    depth = slab_depth * slabs
    slab_height = height // slabs
    rows = channels * height
    voxels = depth * height * width
    factor = 1.0 / math.sqrt(lax.axis_size("dp") * voxels)
    me = jnp.stack([lax.axis_index("space"), lax.axis_index("dp"), lax.axis_index("section")]).astype(jnp.int32)

    shape = pltpu.VMEM
    size = channels * slab_depth * height
    far, near = slabs // 2, slabs // 4
    enc_raw, cot_raw, dec_raw, deep_raw = (
        cells.reshape(size, width) for cells in (enc_input, dec_cotangent, dec_input, deep_cotangent)
    )
    enc_far = swapped(enc_raw, far)
    enc_near = swapped(enc_raw, near)

    square = shape((size, size), BF16)
    matrix = shape((TAPS * rows, TAPS * rows), BF16)
    small = pltpu.VMEM((1, channels), F32)
    wide = pltpu.VMEM((enc_weight.shape[1], channels, 128), F32)
    enc_banded, turn, back, columns, enc_own, mine, dec_taps = call(
        prepare_kernel,
        (
            matrix, square, square, shape((4, channels, 128), F32), shape((size, width), BF16),
            shape((3 * size, width), BF16), shape(dec_weight.shape[1:], BF16),
        ),
        [
            pltpu.VMEM(enc_weight.shape[1:], BF16), small, small, small, small,
            pltpu.SemaphoreType.DMA((10,)), wide,
        ],
        1,
        [pl.BlockSpec(memory_space=pltpu.HBM)] * 10 + [pl.BlockSpec(memory_space=pltpu.SMEM)],
    )(
        *(
            pltpu.with_memory_space_constraint(array, pltpu.HBM)
            for array in (
                enc_weight[0], dec_weight[0], enc_gain, enc_bias, dec_gain, dec_bias,
                enc_raw, cot_raw, dec_raw, deep_raw,
            )
        ),
        me,
    )
    pair_far = swapped(mine[: 2 * size], far)
    others_near = swapped(mine, near)
    enc_relay = swapped(enc_far, near)
    flip_banded, up_banded, down_banded = call(weights_kernel, (matrix, matrix, matrix), [wide])(dec_taps)
    pair_relay = swapped(pair_far, near)

    shifted_shape = (depth, TAPS * rows, width)
    cell_shape = (depth, rows, width)
    turned = pltpu.VMEM((size, slabs * width), BF16)
    parts = pltpu.VMEM((depth + 2, TAPS, rows, width), F32)
    padded = pltpu.VMEM((depth + 2, rows + 2 * channels, width), BF16)
    pre, line_sums = pltpu.VMEM(cell_shape, F32), pltpu.VMEM((2, rows, width), F32)
    channel_sums = pltpu.VMEM((2, channels, width), F32)
    enc_shifted, hat, skip, skip_own, scale = call(
        functools.partial(enc_kernel, channels),
        (
            shape(shifted_shape, BF16),
            shape(cell_shape, F32),
            shape(cell_shape, BF16),
            shape((size, width), BF16),
            shape((channels, 128), F32),
        ),
        [turned, parts, pre, channel_sums],
    )(me, enc_own, enc_near, enc_far, enc_relay, enc_banded, turn, columns)
    deep_far = swapped(lax.optimization_barrier((deep_raw, scale))[0], far)
    deep_relay = swapped(deep_far, near)
    skip_grad, cot = call(
        functools.partial(skip_grad_kernel, size),
        (shape(cell_shape, BF16), shape(cell_shape, BF16)),
        [pltpu.VMEM(shifted_shape, BF16), turned, parts],
        1,
    )(me, mine, others_near, pair_far, pair_relay, flip_banded, turn, scale)

    first, second, up, down = call(
        functools.partial(dec_kernel, channels, size),
        (shape((size, width), BF16),) * 2 + (shape(shifted_shape, BF16),) * 2,
        [turned, parts, pre, channel_sums],
        1,
    )(
        me, mine, others_near, pair_far, pair_relay, skip, up_banded, down_banded, turn, columns,
        skip_own, skip_grad,
    )
    first = paired(first, 0)

    flat_rows = TAPS * TAPS * TAPS * channels * channels // 128
    pair = halves(flat_rows) and halves(2 * flat_rows)

    dec_rows, enc_rows = 2 * flat_rows // (PAIR * slabs), flat_rows // (PAIR * slabs)
    both_rows = padded_rows(dec_rows) + padded_rows(enc_rows)

    def grad_shapes(total):
        if not pair:
            return (shape((total, 128), F32),)
        return (shape((total // (PAIR * slabs), 128), F32),) * 2

    def grad_scratch(total, tiles):
        outers = 2 * PAIR if pair else TAPS * TAPS
        held = total // (TAPS * TAPS) * outers
        return [padded, pltpu.VMEM((tiles, outers * channels, 128), F32), pltpu.VMEM((held, 128), F32)]

    dec_flat = call(
        functools.partial(dec_grad_kernel, channels, factor, slabs),
        grad_shapes(2 * flat_rows),
        grad_scratch(2 * flat_rows, 2),
    )(me, cot, up, down)
    second = paired(lax.optimization_barrier((second, dec_flat[0]))[0], 1)
    enc_flat = call(
        functools.partial(enc_grad_kernel, channels, factor, slabs),
        (shape((both_rows, 128), F32), shape((both_rows, 128), BF16))
        if pair
        else grad_shapes(flat_rows),
        [turned, pre, line_sums, *grad_scratch(flat_rows, 1)],
        0 if pair else 1,
    )(
        me, mine, others_near, deep_far, deep_relay, turn, skip_grad, hat, scale, columns, enc_shifted,
        *dec_flat,
    )

    moved = jax.ShapeDtypeStruct((size, width), BF16)
    enc_handoff, dec_handoff = call(
        functools.partial(put_kernel, lax.axis_size("section")), (moved, moved), [], 1
    )(me, back, first, second, enc_flat[0])
    if pair:
        kept, sent = enc_flat
        received = lax.ppermute(sent, "dp", [(0, 1), (1, 0)])
        ends = tuple(jax.ShapeDtypeStruct((1, count * 128), F32) for count in (dec_rows, enc_rows))
        grads = call(finish_kernel, ends, [])(kept, received)
    else:
        grads = [scattered(dec_flat[0]), scattered(enc_flat[0])]
    enc_handoff = enc_handoff.reshape(1, 1, channels, slab_depth, height, width)
    dec_handoff = dec_handoff.reshape(1, 1, channels, depth, slab_height, width)
    return (enc_handoff, dec_handoff, grads[1].reshape(1, -1), grads[0].reshape(1, -1))


def solution(mesh):
    in_specs = (
        P("section", "dp", None, "space", None, None),
        P("section", "dp", None, None, "space", None),
        P("section", "dp", None, None, "space", None),
        P("section", "dp", None, "space", None, None),
        P("section", None, None, None),
        P("section", None, None, None),
        P("section", None),
        P("section", None),
        P("section", None),
        P("section", None),
    )
    out_specs = (
        P("section", "dp", None, "space", None, None),
        P("section", "dp", None, None, "space", None),
        P("section", ("dp", "space")),
        P("section", ("dp", "space")),
    )

    return jax.shard_map(body, mesh=mesh, in_specs=in_specs, out_specs=out_specs, check_vma=False)
```
